32 devices in a mesh: grp: 2 (over x), dom: 4 (over y, core), pen: 4 (over z).
Axes of the slice: x: 2, y: 2, z: 4, core: 2. Of those that a mesh axis runs over, the one named last changes fastest.
Arguments:
- atoms: float32 [4, 2, 4, 16384], P(None, 'grp', 'dom', 'pen'), may hold values from -6 to 6, as said below
- pair_home: int32 [2, 4, 256], P('grp', 'dom', 'pen'), may hold values from 0 to 31
- pair_other: int32 [2, 4, 256], P('grp', 'dom', 'pen'), may hold values from 0 to 287
Outputs:
- short_forces: float32 [3, 2, 4, 16384], P(None, 'grp', 'dom', 'pen')
- long_forces: float32 [3, 2, 4, 16384], P(None, 'grp', 'dom', 'pen')
The draws below stay inside these ranges and needn't reach their ends.
Inputs may be any that keep to these rules, and one draw needn't show every extreme that they name: `atoms`: in block (g, d, p) the first coordinate lies in [d / 4, (d + 0.98) / 4), the second in [p / 4, (p + 0.98) / 4), the third in [0, 1); the fourth component is the charge, within -6 to 6.
All inputs are finite; a program needn't handle non-finite values.
Results may differ from the reference program's by a relative error of at most 0.0003.
Values sent between devices are 32-bit elements; how exact they have to be, the bound alone decides.
No kernel may reach another device: no remote copies, remote signals or barrier semaphores. Data moves between devices by JAX's collectives and lax.ppermute only.
A program may use at most 64 MiB of HBM per device.

```python
import math
import jax
import jax.numpy as jnp
from jax import lax

NG = 128
TILE = 128
A_DEV = 4096
PAIRS_DEV = 64
N_GRP = 2
N_DOM = 4
N_PEN = 4


def draw_atoms(key, part):
    subkeys = jax.random.split(jax.random.fold_in(key, 11), 4)
    shape = (N_GRP, N_DOM, N_PEN, A_DEV)
    dom_ids = lax.broadcasted_iota(jnp.float32, shape, 1)
    pen_ids = lax.broadcasted_iota(jnp.float32, shape, 2)
    coord_x = (dom_ids + 0.98 * jax.random.uniform(subkeys[0], shape, jnp.float32)) / N_DOM
    coord_y = (pen_ids + 0.98 * jax.random.uniform(subkeys[1], shape, jnp.float32)) / N_PEN
    coord_z = 0.999 * jax.random.uniform(subkeys[2], shape, jnp.float32)
    charge = jnp.clip(jax.random.normal(subkeys[3], shape, jnp.float32), -4.0, 4.0)
    stacked = jnp.stack([coord_x, coord_y, coord_z, charge])
    return stacked.reshape(4, N_GRP, N_DOM, N_PEN * A_DEV)


def place_ends(values, own_key, least, top_value):
    spot = [jax.random.randint(jax.random.fold_in(own_key, axis), (), 0, length) for axis, length in enumerate(values.shape)]
    widest = values.shape.index(max(values.shape))
    beside = spot[:widest] + [(spot[widest] + 1) % values.shape[widest]] + spot[widest + 1:]
    return values.at[tuple(spot)].set(least).at[tuple(beside)].set(top_value)


def setup_inputs(seed: int = 0) -> dict:
    key_list = jax.random.split(jax.random.key(seed), 4)
    atoms = draw_atoms(jax.random.fold_in(key_list[3], 71), 0)
    pair_home = place_ends(jax.random.randint(key_list[1], (N_GRP, N_DOM, N_PEN * PAIRS_DEV), 0, A_DEV // TILE), jax.random.fold_in(key_list[1], 1), 0, (A_DEV // TILE) - 1).astype(jnp.int32)
    pair_other = place_ends(jax.random.randint(key_list[2], (N_GRP, N_DOM, N_PEN * PAIRS_DEV), 0, 9 * (A_DEV // TILE)), jax.random.fold_in(key_list[2], 1), 0, (9 * (A_DEV // TILE)) - 1).astype(jnp.int32)
    return {"atoms": atoms, "pair_home": pair_home, "pair_other": pair_other}


def spline_terms(scaled):
    floored = jnp.floor(scaled)
    fraction = scaled - floored
    remain = 1.0 - fraction
    frac_sq = fraction * fraction
    frac_cube = frac_sq * fraction
    thetas = [remain * remain * remain / 6.0, (3.0 * frac_cube - 6.0 * frac_sq + 4.0) / 6.0, (-3.0 * frac_cube + 3.0 * frac_sq + 3.0 * fraction + 1.0) / 6.0, frac_cube / 6.0]
    slopes = [-0.5 * remain * remain, 1.5 * frac_sq - 2.0 * fraction, -1.5 * frac_sq + fraction + 0.5, 0.5 * frac_sq]
    return (floored.astype(jnp.int32) - 3, thetas, slopes)

def pair_push(home_pos, other_pos, scales):
    displace = home_pos[:, :3, :, None] - other_pos[:, :3, None, :]
    displace = displace - jnp.floor(displace + 0.5)
    scaled = displace * scales[None, :, None, None]
    weight = jnp.exp(-0.5 * lax.optimization_barrier(jnp.sum(scaled * scaled, axis=1))) * other_pos[:, 3, None, :]
    return lax.optimization_barrier(jnp.sum(scaled * weight[:, None], axis=3)) * home_pos[:, 3:4, :]

def green_factor(freq_x, freq_y, freq_z, grid_cells):

    def signed(frequencies):
        return jnp.where(frequencies < grid_cells // 2, frequencies, frequencies - grid_cells)

    def modulus(frequencies):
        turned = 2.0 * jnp.pi * signed(frequencies).astype(jnp.float32) / grid_cells
        ratio = (2.0 + jnp.cos(turned)) / 3.0
        return 1.0 / (ratio * ratio)
    signed_x = signed(freq_x)
    signed_y = signed(freq_y)
    signed_z = signed(freq_z)
    square = (signed_x * signed_x + signed_y * signed_y + signed_z * signed_z).astype(jnp.float32)
    beta = 0.6 * grid_cells
    safe = jnp.maximum(square, 1.0)
    value = jnp.exp(-jnp.pi * jnp.pi * square / (beta * beta)) / (jnp.pi * safe)
    value = value * modulus(freq_x) * modulus(freq_y) * modulus(freq_z)
    return jnp.where(square > 0.5, value, 0.0)

def reference(atoms, pair_home, pair_other):
    grid_cells = NG
    tile_count = A_DEV // TILE
    blocks = atoms.reshape(4, N_GRP, N_DOM, N_PEN, A_DEV)
    shifted = []
    for step_dom in (1, 0, -1):
        for step_pen in (1, 0, -1):
            shifted.append(jnp.roll(jnp.roll(blocks, step_dom, axis=2), step_pen, axis=3))
    nearby = jnp.stack(shifted).transpose(2, 3, 4, 0, 1, 5).reshape(N_GRP * N_DOM * N_PEN, 9, 4, A_DEV)
    homes = pair_home.reshape(-1, PAIRS_DEV)
    others = pair_other.reshape(-1, PAIRS_DEV)
    scales = jnp.array([2.0 * N_DOM, 2.0 * N_PEN, 2.0 * N_DOM], jnp.float32)

    def one_block(inputs):
        around, home_ids, other_ids = inputs
        tiled = around.reshape(9, 4, tile_count, TILE).transpose(0, 2, 1, 3).reshape(9 * tile_count, 4, TILE)
        own_tiles = tiled[4 * tile_count:5 * tile_count]
        pushes = pair_push(own_tiles[home_ids], tiled[other_ids], scales)
        totals = jnp.zeros((tile_count, 3, TILE), pushes.dtype).at[home_ids].add(pushes)
        return totals.transpose(1, 0, 2).reshape(3, A_DEV)
    short_out = lax.map(one_block, (nearby, homes, others))
    short_out = short_out.transpose(1, 0, 2).reshape(3, N_GRP, N_DOM, N_PEN * A_DEV)
    short_out = short_out * (2.0 / math.sqrt(A_DEV / N_DOM))
    flat = atoms.reshape(4, -1)
    charge = flat[3]
    terms = [spline_terms(flat[axis_id] * grid_cells) for axis_id in range(3)]
    corner = jnp.arange(4, dtype=jnp.int32)
    z_ids = jnp.mod(terms[2][0][:, None] + corner[None, :], grid_cells)
    z_weights = jnp.stack(terms[2][1], axis=1)
    z_slopes = jnp.stack(terms[2][2], axis=1)
    charge_mesh = jnp.zeros((grid_cells, grid_cells, grid_cells), flat.dtype)
    for step_x in range(4):
        x_ids = jnp.mod(terms[0][0] + step_x, grid_cells)
        for step_y in range(4):
            y_ids = jnp.mod(terms[1][0] + step_y, grid_cells)
            amount = (charge * terms[0][1][step_x] * terms[1][1][step_y])[:, None] * z_weights
            charge_mesh = charge_mesh.at[x_ids[:, None], y_ids[:, None], z_ids].add(amount)
    frequencies = jnp.arange(grid_cells, dtype=jnp.int32)
    green = green_factor(frequencies[:, None, None], frequencies[None, :, None], frequencies[None, None, :], grid_cells)
    potential = jnp.real(jnp.fft.ifftn(jnp.fft.fftn(charge_mesh) * green)) * float(grid_cells) ** 3
    grads = [jnp.zeros_like(charge) for axis_id in range(3)]
    for step_x in range(4):
        x_ids = jnp.mod(terms[0][0] + step_x, grid_cells)
        for step_y in range(4):
            y_ids = jnp.mod(terms[1][0] + step_y, grid_cells)
            picked = potential[x_ids[:, None], y_ids[:, None], z_ids]
            along_z = lax.optimization_barrier(jnp.sum(picked * z_weights, axis=1))
            slope_z = lax.optimization_barrier(jnp.sum(picked * z_slopes, axis=1))
            grads[0] = grads[0] + terms[0][2][step_x] * terms[1][1][step_y] * along_z
            grads[1] = grads[1] + terms[0][1][step_x] * terms[1][2][step_y] * along_z
            grads[2] = grads[2] + terms[0][1][step_x] * terms[1][1][step_y] * slope_z
    total_atoms = A_DEV * N_GRP * N_DOM * N_PEN
    long_scale = -0.4 * grid_cells / math.sqrt(grid_cells * total_atoms)
    long_out = (jnp.stack(grads) * charge[None, :] * long_scale).reshape(3, N_GRP, N_DOM, N_PEN * A_DEV)
    return (short_out, long_out)
```

```python
import math

import jax
import jax.numpy as jnp
import numpy as np
from jax import lax
from jax.experimental import pallas as pl
from jax.experimental.pallas import tpu as pltpu
from jax.sharding import PartitionSpec as P

NG = 128
TILE = 128


exact_precision = lax.Precision.HIGHEST


def with_halo(block, sides, width):
    for axis, dim in sides:
        count = lax.axis_size(axis)
        forward = [(i, i + 1) for i in range(count - 1)]
        forward.append((count - 1, 0))
        backward = [(target, source) for source, target in forward]
        low = lax.ppermute(
            lax.slice_in_dim(block, block.shape[dim] - width, None, axis=dim), axis, forward
        )
        high = lax.ppermute(lax.slice_in_dim(block, 0, width, axis=dim), axis, backward)
        block = jnp.concatenate([low, block, high], axis=dim)
    return block


def passed_along(block, axis, distance):
    devices = range(lax.axis_size(axis))
    route = [((i - distance) % len(devices), i) for i in devices]
    return lax.ppermute(block, axis, route)


def matmul(left, right):
    return jnp.dot(left, right, precision=exact_precision, preferred_element_type=jnp.float32)


def spline_terms(scaled):
    floored = jnp.floor(scaled)
    fraction = scaled - floored
    remain = 1.0 - fraction
    frac_sq = fraction * fraction
    frac_cube = frac_sq * fraction
    thetas = [
        remain * remain * remain / 6.0,
        (3.0 * frac_cube - 6.0 * frac_sq + 4.0) / 6.0,
        (-3.0 * frac_cube + 3.0 * frac_sq + 3.0 * fraction + 1.0) / 6.0,
        frac_cube / 6.0,
    ]
    slopes = [
        -0.5 * remain * remain,
        1.5 * frac_sq - 2.0 * fraction,
        -1.5 * frac_sq + fraction + 0.5,
        0.5 * frac_sq,
    ]
    return (floored.astype(jnp.int32) - 3, thetas, slopes)


def spline_rows(coords, anchor, planes, grid_cells):
    lowest, thetas, slopes = spline_terms(coords * grid_cells)
    plane_ids = lax.broadcasted_iota(jnp.int32, (planes, 1), 0)
    values = jnp.zeros((planes, coords.shape[0]), jnp.float32)
    slopes_out = jnp.zeros_like(values)
    for offset in range(4):
        matches = (jnp.mod(lowest + offset - anchor, grid_cells)[None, :] == plane_ids).astype(
            jnp.float32
        )
        values = values + matches * thetas[offset][None, :]
        slopes_out = slopes_out + matches * slopes[offset][None, :]
    return (values, slopes_out)


def pair_push(home_pos, other_pos, scales):
    displace = home_pos[:, :3, :, None] - other_pos[:, :3, None, :]
    displace = displace - jnp.floor(displace + 0.5)
    scaled = displace * scales[None, :, None, None]
    weight = jnp.exp(-0.5 * jnp.sum(scaled * scaled, axis=1)) * other_pos[:, 3, None, :]
    return jnp.sum(scaled * weight[:, None], axis=3) * home_pos[:, 3:4, :]


def green_factor(freq_x, freq_y, freq_z, grid_cells):

    def signed(frequencies):
        return jnp.where(frequencies < grid_cells // 2, frequencies, frequencies - grid_cells)

    def modulus(frequencies):
        turned = 2.0 * jnp.pi * signed(frequencies).astype(jnp.float32) / grid_cells
        ratio = (2.0 + jnp.cos(turned)) / 3.0
        return 1.0 / (ratio * ratio)

    signed_x = signed(freq_x)
    signed_y = signed(freq_y)
    signed_z = signed(freq_z)
    square = (signed_x * signed_x + signed_y * signed_y + signed_z * signed_z).astype(jnp.float32)
    beta = 0.6 * grid_cells
    safe = jnp.maximum(square, 1.0)
    value = jnp.exp(-jnp.pi * jnp.pi * square / (beta * beta)) / (jnp.pi * safe)
    value = value * modulus(freq_x) * modulus(freq_y) * modulus(freq_z)
    return jnp.where(square > 0.5, value, 0.0)


def phase_tables(frequencies, cell_ids, grid_cells):
    turns = jnp.mod(frequencies[:, None] * cell_ids[None, :], grid_cells).astype(jnp.float32)
    angle = turns * (2.0 * jnp.pi / grid_cells)
    return (jnp.cos(angle), jnp.sin(angle))


def spread_mesh(spread_atoms, first_x, first_y, slab_cells, column, grid_cells):
    span_size = min(1024, spread_atoms.shape[1])
    batches = spread_atoms.reshape(4, -1, span_size).transpose(1, 0, 2)

    def spread_step(totals, atom_batch):
        weight_x, unused_x = spline_rows(atom_batch[0], first_x, slab_cells, grid_cells)
        weight_y, unused_y = spline_rows(atom_batch[1], first_y, column, grid_cells)
        weight_z, unused_z = spline_rows(atom_batch[2], 0, grid_cells, grid_cells)
        weighted_y = weight_y * atom_batch[3][None, :]
        paired = weight_x[:, None, :] * weighted_y[None, :, :]
        paired = paired.reshape(slab_cells * column, span_size)
        product = lax.dot_general(
            paired,
            weight_z,
            (((1,), (1,)), ((), ())),
            precision=exact_precision,
            preferred_element_type=jnp.float32,
        )
        return (totals + product, None)

    totals, unused = lax.scan(
        spread_step, jnp.zeros((slab_cells * column, grid_cells), jnp.float32), batches
    )
    return totals


def forward_lines(cos_tab, sin_tab, real_part, imag_part):
    return (
        matmul(cos_tab, real_part) + matmul(sin_tab, imag_part),
        matmul(cos_tab, imag_part) - matmul(sin_tab, real_part),
    )


def inverse_lines(cos_tab, sin_tab, real_part, imag_part):
    return (
        matmul(cos_tab, real_part) - matmul(sin_tab, imag_part),
        matmul(cos_tab, imag_part) + matmul(sin_tab, real_part),
    )


def on_device(atoms, pair_home, pair_other):
    grid_cells = NG
    groups = lax.axis_size("grp")
    domains = lax.axis_size("dom")
    pencils = lax.axis_size("pen")
    slab_cells = grid_cells // domains
    column = grid_cells // pencils
    atom_count = atoms.shape[3]
    tile_count = atom_count // TILE
    dom_at = lax.axis_index("dom")
    pen_at = lax.axis_index("pen")
    grp_at = lax.axis_index("grp")
    first_x = dom_at * slab_cells
    first_y = pen_at * column
    local_atoms = atoms.reshape(1, 1, 4 * atom_count)
    nearby = with_halo(local_atoms, (("dom", 0), ("pen", 1)), 1)
    nearby = nearby.reshape(3, 3, 4, atom_count)
    tiled = (
        nearby.reshape(9, 4, tile_count, TILE)
        .transpose(0, 2, 1, 3)
        .reshape(9 * tile_count, 4, TILE)
    )
    own_tiles = tiled[4 * tile_count : 5 * tile_count]
    home_ids = pair_home.reshape(-1)
    other_ids = pair_other.reshape(-1)
    pair_count = home_ids.shape[0]
    scales = jnp.array([2.0 * domains, 2.0 * pencils, 2.0 * domains], jnp.float32)

    def pair_group(id_pair):
        home_blk, other_blk = id_pair
        return pair_push(own_tiles[home_blk], tiled[other_blk], scales)

    pushes = lax.map(pair_group, (home_ids.reshape(-1, 16), other_ids.reshape(-1, 16)))
    pushes = pushes.reshape(pair_count, 3 * TILE)
    owners = (home_ids[:, None] == lax.broadcasted_iota(jnp.int32, (1, tile_count), 1)).astype(
        jnp.float32
    )
    summed = lax.dot_general(
        owners,
        pushes,
        (((0,), (0,)), ((), ())),
        precision=exact_precision,
        preferred_element_type=jnp.float32,
    )
    short_out = summed.reshape(tile_count, 3, TILE).transpose(1, 0, 2).reshape(3, 1, 1, atom_count)
    short_out = short_out * (2.0 / math.sqrt(atom_count / domains))
    spread_atoms = nearby[1:3, 1:3].transpose(2, 0, 1, 3).reshape(4, 4 * atom_count)
    z_ids = lax.iota(jnp.int32, grid_cells)
    cos_z, sin_z = phase_tables(z_ids, z_ids, grid_cells)
    charge_mesh = spread_mesh(spread_atoms, first_x, first_y, slab_cells, column, grid_cells)
    kz_rows = grid_cells // groups
    kz_part = kz_rows // domains
    kx_part = grid_cells // pencils
    z_real = matmul(charge_mesh, cos_z)
    z_imag = -matmul(charge_mesh, sin_z)
    sum_real, sum_imag = (
        lax.psum_scatter(z_real, "grp", scatter_dimension=1, tiled=True),
        lax.psum_scatter(z_imag, "grp", scatter_dimension=1, tiled=True),
    )
    sum_real = sum_real.reshape(slab_cells, column, kz_rows)
    sum_imag = sum_imag.reshape(slab_cells, column, kz_rows)
    line_real, line_imag = (
        lax.all_to_all(sum_real, "dom", split_axis=2, concat_axis=0, tiled=True),
        lax.all_to_all(sum_imag, "dom", split_axis=2, concat_axis=0, tiled=True),
    )
    fx_real, fx_imag = forward_lines(
        cos_z,
        sin_z,
        line_real.reshape(grid_cells, column * kz_part),
        line_imag.reshape(grid_cells, column * kz_part),
    )
    fx_real = fx_real.reshape(grid_cells, column, kz_part)
    fx_imag = fx_imag.reshape(grid_cells, column, kz_part)
    ylin_real, ylin_imag = (
        lax.all_to_all(fx_real, "pen", split_axis=0, concat_axis=1, tiled=True),
        lax.all_to_all(fx_imag, "pen", split_axis=0, concat_axis=1, tiled=True),
    )
    ylin_real = ylin_real.transpose(1, 0, 2).reshape(grid_cells, kx_part * kz_part)
    ylin_imag = ylin_imag.transpose(1, 0, 2).reshape(grid_cells, kx_part * kz_part)
    fy_real, fy_imag = forward_lines(cos_z, sin_z, ylin_real, ylin_imag)
    kx_ids = pen_at * kx_part + lax.iota(jnp.int32, kx_part)
    kz_ids = grp_at * kz_rows + dom_at * kz_part + lax.iota(jnp.int32, kz_part)
    factor = green_factor(
        kx_ids[None, :, None], z_ids[:, None, None], kz_ids[None, None, :], grid_cells
    )
    factor = factor.reshape(grid_cells, kx_part * kz_part)
    iy_real, iy_imag = inverse_lines(cos_z, sin_z, fy_real * factor, fy_imag * factor)
    iy_real = iy_real.reshape(grid_cells, kx_part, kz_part).transpose(1, 0, 2)
    iy_imag = iy_imag.reshape(grid_cells, kx_part, kz_part).transpose(1, 0, 2)
    back_real, back_imag = (
        lax.all_to_all(iy_real, "pen", split_axis=1, concat_axis=0, tiled=True),
        lax.all_to_all(iy_imag, "pen", split_axis=1, concat_axis=0, tiled=True),
    )
    ix_real, ix_imag = inverse_lines(
        cos_z,
        sin_z,
        back_real.reshape(grid_cells, column * kz_part),
        back_imag.reshape(grid_cells, column * kz_part),
    )
    ix_real = ix_real.reshape(grid_cells, column, kz_part)
    ix_imag = ix_imag.reshape(grid_cells, column, kz_part)
    slab_real, slab_imag = (
        lax.all_to_all(ix_real, "dom", split_axis=0, concat_axis=2, tiled=True),
        lax.all_to_all(ix_imag, "dom", split_axis=0, concat_axis=2, tiled=True),
    )
    whole_real, whole_imag = (
        lax.all_gather(slab_real, "grp", axis=2, tiled=True),
        lax.all_gather(slab_imag, "grp", axis=2, tiled=True),
    )
    own_pot = matmul(whole_real.reshape(-1, grid_cells), cos_z) - matmul(
        whole_imag.reshape(-1, grid_cells), sin_z
    )
    own_pot = own_pot.reshape(slab_cells, column, grid_cells)
    lower_planes = passed_along(own_pot[slab_cells - 3 :], "dom", 1)
    taller = jnp.concatenate([lower_planes, own_pot], axis=0)
    side_planes = passed_along(taller[:, column - 3 :], "pen", 1)
    rimmed = jnp.concatenate([side_planes, taller], axis=1)
    flat_pot = rimmed.transpose(1, 0, 2).reshape(-1, grid_cells)
    batch_size = min(256, atom_count)
    own_atoms = atoms.reshape(4, -1, batch_size).transpose(1, 0, 2)

    def interpolate(atom_batch):
        weight_x, slope_x = spline_rows(atom_batch[0], first_x - 3, slab_cells + 3, grid_cells)
        weight_y, slope_y = spline_rows(atom_batch[1], first_y - 3, column + 3, grid_cells)
        weight_z, slope_zw = spline_rows(atom_batch[2], 0, grid_cells, grid_cells)
        along_z = matmul(flat_pot, weight_z).reshape(column + 3, slab_cells + 3, batch_size)
        slope_z = matmul(flat_pot, slope_zw).reshape(column + 3, slab_cells + 3, batch_size)
        grad_x = jnp.sum(weight_y[:, None] * slope_x[None] * along_z, axis=(0, 1))
        grad_y = jnp.sum(slope_y[:, None] * weight_x[None] * along_z, axis=(0, 1))
        grad_z = jnp.sum(weight_y[:, None] * weight_x[None] * slope_z, axis=(0, 1))
        return jnp.stack([grad_x, grad_y, grad_z]) * atom_batch[3][None, :]

    gradients = lax.map(interpolate, own_atoms)
    gradients = gradients.transpose(1, 0, 2).reshape(3, 1, 1, atom_count)
    total_atoms = atom_count * groups * domains * pencils
    long_scale = -0.4 * grid_cells / math.sqrt(grid_cells * total_atoms)
    return (short_out, gradients * long_scale)


LANES = 128
SUBLANES = 8
MESH_AXES = ("pen", "grp", "dom")


def fast_sizes(groups, domains, pencils, atom_count):
    devices = groups * domains * pencils
    if NG != LANES or NG % devices or NG // domains != 32 or NG // pencils != 32:
        return None
    share = NG // devices
    if (domains * share) % SUBLANES or atom_count % 512 or TILE != LANES:
        return None
    slab = NG // domains
    column = NG // pencils
    return dict(
        share=share,
        slab=slab,
        stride=column + 4,
        column=column,
        rows=-(-(slab + 3) * (column + 4) // LANES) * LANES,
        block=domains * share,
        groups=groups,
        domains=domains,
        pencils=pencils,
    )


def real_basis():
    freq = np.arange(NG)
    freq = np.where(freq <= NG // 2, freq, freq - NG // 2)
    turns = (freq[:, None] * np.arange(NG)[None, :]) % NG
    angle = turns * (2.0 * np.pi / NG)
    use_cos = (np.arange(NG) <= NG // 2)[:, None]
    return freq, np.where(use_cos, np.cos(angle), np.sin(angle)).astype(np.float32)


def line_factor(freq):
    beta = 0.6 * NG
    ratio = (2.0 + np.cos(2.0 * np.pi * freq / NG)) / 3.0
    count = np.where((freq == 0) | (freq == NG // 2), 1.0, 2.0)
    return count * np.exp(-np.pi * np.pi * freq * freq / (beta * beta)) / (ratio * ratio)


def split_bf16(value):
    high = value.astype(jnp.bfloat16)
    low = (value - high.astype(jnp.float32)).astype(jnp.bfloat16)
    return high, low


def choose(place, options):
    out = jnp.where(place == 0.0, options[0], 0.0)
    for k in range(1, 4):
        out = jnp.where(place == float(k), options[k], out)
    return out


def row_ids(count, lanes):
    return lax.broadcasted_iota(jnp.int32, (count, lanes), 0).astype(jnp.float32)


def spline_parts(coord):
    scaled = coord * float(NG)
    floored = jnp.floor(scaled)
    fraction = scaled - floored
    remain = 1.0 - fraction
    frac_sq = fraction * fraction
    frac_cube = frac_sq * fraction
    sixth = 1.0 / 6.0
    thetas = [
        remain * remain * remain * sixth,
        (3.0 * frac_cube - 6.0 * frac_sq + 4.0) * sixth,
        (-3.0 * frac_cube + 3.0 * frac_sq + 3.0 * fraction + 1.0) * sixth,
        frac_cube * sixth,
    ]
    slopes = [
        -0.5 * remain * remain,
        1.5 * frac_sq - 2.0 * fraction,
        -1.5 * frac_sq + fraction + 0.5,
        0.5 * frac_sq,
    ]
    return floored, thetas, slopes


def z_place(floored, lanes):
    place = row_ids(NG, lanes) - floored + 3.0
    return jnp.where(place >= float(NG), place - float(NG), place)


def spread_kernel(first_ref, basis_ref, atoms_ref, out_ref, acc_ref, high_ref, low_ref, *, sizes):
    step = pl.program_id(0)
    lanes = atoms_ref.shape[1]
    rows, stride = sizes["rows"], sizes["stride"]
    floor_x, theta_x, _ = spline_parts(atoms_ref[0:1, :])
    floor_y, theta_y, _ = spline_parts(atoms_ref[1:2, :])
    floor_z, theta_z, _ = spline_parts(atoms_ref[2:3, :])
    floor_x = floor_x - first_ref[0].astype(jnp.float32)
    floor_y = floor_y - first_ref[1].astype(jnp.float32)
    weight_x = choose(row_ids(stride + 4, lanes) - floor_x, theta_x)
    period = row_ids(2 * stride, lanes)
    period = jnp.where(period >= float(stride), period - float(stride), period)
    weight_y = choose(period - floor_y, theta_y) * atoms_ref[3:4, :]
    weight_z = choose(z_place(floor_z, lanes), theta_z)
    z_high, z_low = split_bf16(weight_z)
    low_half = lax.broadcasted_iota(jnp.int32, (SUBLANES, lanes), 0) < stride % SUBLANES
    whole = stride // SUBLANES * SUBLANES
    for group in range(-(-rows // (4 * stride))):
        pieces = []
        for pair in range(2):
            at = 4 * group + 2 * pair
            if at >= sizes["slab"] + 4:
                continue
            first = jnp.broadcast_to(weight_x[at : at + 1, :], (SUBLANES, lanes))
            second = jnp.broadcast_to(weight_x[at + 1 : at + 2, :], (SUBLANES, lanes))
            mixed = jnp.where(low_half, first, second)
            for tile in range(2 * stride // SUBLANES):
                factor = first if tile < whole // SUBLANES else second
                factor = mixed if tile == whole // SUBLANES else factor
                pieces.append(factor * weight_y[tile * SUBLANES : (tile + 1) * SUBLANES, :])
        start = group * 4 * stride
        count = min(4 * stride, rows - start)
        paired = jnp.concatenate(pieces, axis=0)[:count]
        high, low = split_bf16(paired)
        high_ref[start : start + count, :] = high
        low_ref[start : start + count, :] = low
    contract = (((1,), (1,)), ((), ()))
    both = jnp.concatenate([z_high, z_low], axis=0)
    main = lax.dot_general(high_ref[...], both, contract, preferred_element_type=jnp.float32)
    rest = lax.dot_general(low_ref[...], z_high, contract, preferred_element_type=jnp.float32)
    total = main[:, :NG] + main[:, NG:] + rest

    @pl.when(step == 0)
    def _():
        acc_ref[...] = total

    @pl.when(step > 0)
    def _():
        acc_ref[...] += total

    @pl.when(step == pl.num_programs(0) - 1)
    def _():
        out_ref[...] = lax.dot_general(
            basis_ref[...],
            acc_ref[...],
            contract,
            precision=exact_precision,
            preferred_element_type=jnp.float32,
        )


def ring_mask(lane, start, length):
    start = start % LANES
    if start + length <= LANES:
        return (lane >= start) & (lane < start + length)
    return (lane >= start) | (lane < start + length - LANES)


def spectral_kernel(
    line_ref, square_ref, basis_ref, mixed_ref, mixed_t_ref, plane_ref, plane_sq_ref,
    in_ref, out_ref, sum_ref, work_ref, *, sizes
):
    block, share, stride = sizes["block"], sizes["share"], sizes["stride"]
    slab, column, groups = sizes["slab"], sizes["column"], sizes["groups"]
    pencils, rows = sizes["pencils"], sizes["rows"]
    for pen in range(pencils):
        total = in_ref[pen * groups * block : (pen * groups + 1) * block, :]
        for grp in range(1, groups):
            start = (pen * groups + grp) * block
            total = total + in_ref[start : start + block, :]
        sum_ref[pen * block : (pen + 1) * block, :] = total
    lane = lax.broadcasted_iota(jnp.int32, (block, LANES), 1)
    width = column + 3

    def gathered(x):
        total = None
        for pen in range(pencils):
            shift = (column * pen - 3 - stride * x) % LANES
            for tile in range(stride * x // LANES, (stride * x + width - 1) // LANES + 1):
                low = max(0, tile * LANES - stride * x)
                high = min(width, (tile + 1) * LANES - stride * x)
                part = sum_ref[pen * block : (pen + 1) * block, tile * LANES : (tile + 1) * LANES]
                part = pltpu.roll(part, shift, 1) if shift else part
                mask = ring_mask(lane, column * pen - 3 + low, high - low)
                part = jnp.where(mask, part, 0.0)
                total = part if total is None else total + part
        return total

    for x in range(slab):
        value = gathered(x + 3)
        if x >= slab - 3:
            value = value + pltpu.roll(gathered(x + 3 - slab), block - share, 0)
        work_ref[x * block : (x + 1) * block, :] = value

    def dot(left, right, contract=(1, 0)):
        return lax.dot_general(
            left,
            right,
            (((contract[0],), (contract[1],)), ((), ())),
            precision=exact_precision,
            preferred_element_type=jnp.float32,
        )

    work_ref[...] = dot(work_ref[...], basis_ref[...], (1, 1))
    for kz in range(share):
        picked = work_ref[pl.ds(kz, NG, stride=share), :]
        spectrum = dot(mixed_ref[...], picked)
        square = plane_sq_ref[...] + square_ref[kz]
        factor = plane_ref[...] * line_ref[kz] / jnp.maximum(square, 1.0)
        factor = jnp.where(square > 0.5, factor, 0.0)
        work_ref[pl.ds(kz, NG, stride=share), :] = dot(mixed_t_ref[...], spectrum * factor)
    work_ref[...] = dot(work_ref[...], basis_ref[...])

    for pen in range(pencils):
        for tile in range(rows // LANES):
            total = jnp.zeros((block, LANES), jnp.float32)
            for x in range(slab + 3):
                low = max(stride * x, tile * LANES)
                high = min(stride * x + width, (tile + 1) * LANES)
                if low >= high:
                    continue
                if x >= 3:
                    value = work_ref[(x - 3) * block : (x - 2) * block, :]
                else:
                    value = work_ref[(slab - 3 + x) * block : (slab - 2 + x) * block, :]
                    value = pltpu.roll(value, share, 0)
                shift = (stride * x - column * pen + 3) % LANES
                value = pltpu.roll(value, shift, 1) if shift else value
                mask = ring_mask(lane, low - tile * LANES, high - low)
                total = jnp.where(mask, value, total)
            for grp in range(groups):
                start = (pen * groups + grp) * block
                out_ref[start : start + block, tile * LANES : (tile + 1) * LANES] = total


def interpolate_kernel(
    first_ref, basis_ref, coef_ref, atoms_ref, out_ref, pot_ref, along_ref, *, sizes, scale
):
    lanes = atoms_ref.shape[1]
    rows, stride = sizes["rows"], sizes["stride"]

    @pl.when(pl.program_id(0) == 0)
    def _():
        potential = lax.dot_general(
            coef_ref[...],
            basis_ref[...],
            (((0,), (0,)), ((), ())),
            precision=exact_precision,
            preferred_element_type=jnp.float32,
        )
        high, low = split_bf16(potential)
        pot_ref[:, :NG] = high
        pot_ref[:, NG : 2 * NG] = low
        pot_ref[:, 2 * NG :] = high

    floor_x, theta_x, slope_x = spline_parts(atoms_ref[0:1, :])
    floor_y, theta_y, slope_y = spline_parts(atoms_ref[1:2, :])
    floor_z, theta_z, slope_z = spline_parts(atoms_ref[2:3, :])
    floor_x = floor_x - first_ref[0].astype(jnp.float32)
    floor_y = floor_y - first_ref[1].astype(jnp.float32)
    place = z_place(floor_z, lanes)
    columns = []
    for options in (theta_z, slope_z):
        high, low = split_bf16(choose(place, options))
        columns.append(jnp.concatenate([high, high, low], axis=0))
    along_ref[...] = jnp.dot(
        pot_ref[...], jnp.concatenate(columns, axis=1), preferred_element_type=jnp.float32
    )
    place = row_ids(stride + 4, lanes) - floor_x
    weight_x, deriv_x = choose(place, theta_x), choose(place, slope_x)
    period = row_ids(2 * stride, lanes)
    period = jnp.where(period >= float(stride), period - float(stride), period)
    place = period - floor_y
    weight_y, deriv_y = choose(place, theta_y), choose(place, slope_y)
    low_half = lax.broadcasted_iota(jnp.int32, (SUBLANES, lanes), 0) < stride % SUBLANES
    middle = stride // SUBLANES
    grads = [jnp.zeros((SUBLANES, lanes), jnp.float32) for axis in range(3)]
    for at in range(0, sizes["slab"] + 3, 2):
        sums = [[None] * 3 for axis in range(3)]
        for tile in range(2 * stride // SUBLANES):
            row = at * stride + tile * SUBLANES
            if row >= rows:
                continue
            span = slice(tile * SUBLANES, (tile + 1) * SUBLANES)
            along = along_ref[row : row + SUBLANES, :lanes]
            slope = along_ref[row : row + SUBLANES, lanes:]
            kind = 0 if tile < middle else 1 if tile == middle else 2
            terms = (along * weight_y[span, :], along * deriv_y[span, :], slope * weight_y[span, :])
            for axis in range(3):
                held = sums[axis][kind]
                sums[axis][kind] = terms[axis] if held is None else held + terms[axis]
        for axis, table in enumerate((deriv_x, weight_x, weight_x)):
            first = jnp.broadcast_to(table[at : at + 1, :], (SUBLANES, lanes))
            second = jnp.broadcast_to(table[at + 1 : at + 2, :], (SUBLANES, lanes))
            factors = (first, jnp.where(low_half, first, second), second)
            for kind in range(3):
                grads[axis] = grads[axis] + sums[axis][kind] * factors[kind]
    charge = atoms_ref[3:4, :] * scale
    for axis in range(3):
        out_ref[axis : axis + 1, :] = jnp.sum(grads[axis], axis=0, keepdims=True) * charge


def pair_kernel(home_ref, other_ref, wrap_ref, near_ref, out_ref, *, factors, scale):
    tiles = near_ref.shape[2] // TILE
    out_ref[...] = jnp.zeros_like(out_ref)
    centre = near_ref.shape[0] // 2

    def one_pair(n, carry):
        home = home_ref[n]
        other = other_ref[n]
        around = other // tiles
        home_at = pl.ds(pl.multiple_of(home * TILE, TILE), TILE)
        other_at = pl.ds(pl.multiple_of((other - around * tiles) * TILE, TILE), TILE)
        mine = near_ref[centre, :, home_at]
        theirs = near_ref[around, :, other_at]
        turned = jnp.concatenate([theirs, theirs], axis=0).T
        delta_x = (mine[0:1, :] - wrap_ref[0, around]) - turned[:, 0:1]
        delta_y = (mine[1:2, :] - wrap_ref[1, around]) - turned[:, 1:2]
        delta_z = mine[2:3, :] - turned[:, 2:3]
        delta_z = delta_z - jnp.floor(delta_z + 0.5)
        scaled = (delta_x * factors[0], delta_y * factors[1], delta_z * factors[2])
        square = scaled[0] * scaled[0] + scaled[1] * scaled[1] + scaled[2] * scaled[2]
        weight = jnp.exp(-0.5 * square) * turned[:, 3:4]
        charge = mine[3:4, :] * scale
        for axis in range(3):
            push = jnp.sum(scaled[axis] * weight, axis=0, keepdims=True) * charge
            out_ref[axis : axis + 1, home_at] += push
        return carry

    lax.fori_loop(0, home_ref.shape[0], one_pair, 0)


def neighbours(block, domains, pencils):
    found = []
    for step_dom in (-1, 0, 1):
        for step_pen in (-1, 0, 1):
            if step_dom == 0 and step_pen == 0:
                found.append(block)
                continue
            route = [
                ((dom + step_dom) % domains * pencils + (pen + step_pen) % pencils, dom * pencils + pen)
                for dom in range(domains)
                for pen in range(pencils)
            ]
            found.append(lax.ppermute(block, ("dom", "pen"), route))
    return jnp.stack(found)


def whole_spec(shape):
    return pl.BlockSpec(shape, lambda *unused: (0,) * len(shape))


def smem_spec():
    return pl.BlockSpec(memory_space=pltpu.SMEM)


def fast_on_device(atoms, pair_home, pair_other, *, sizes):
    groups, domains, pencils = sizes["groups"], sizes["domains"], sizes["pencils"]
    rows, share, block = sizes["rows"], sizes["share"], sizes["block"]
    slab, column, stride = sizes["slab"], sizes["column"], sizes["stride"]
    devices = groups * domains * pencils
    atom_count = atoms.shape[3]
    own = atoms.reshape(4, atom_count)
    dom_at = lax.axis_index("dom")
    pen_at = lax.axis_index("pen")
    grp_at = lax.axis_index("grp")
    first = jnp.stack([dom_at * slab, pen_at * column]).astype(jnp.int32)
    freq, basis = real_basis()
    order = (np.arange(domains)[None, :] * slab + np.arange(slab)[:, None]).reshape(-1)
    mixed = np.ascontiguousarray(basis[:, order])
    line = line_factor(freq)
    plane = jnp.asarray((line[:, None] * line[None, :] / np.pi).astype(np.float32))
    plane_sq = jnp.asarray((freq[:, None] ** 2 + freq[None, :] ** 2).astype(np.float32))
    basis_arr = jnp.asarray(basis)

    chunk = 512
    parallel = pltpu.CompilerParams(dimension_semantics=("arbitrary",))
    charge = pl.pallas_call(
        lambda *refs: spread_kernel(*refs, sizes=sizes),
        grid=(atom_count // chunk,),
        in_specs=[
            smem_spec(),
            whole_spec((NG, NG)),
            pl.BlockSpec((4, chunk), lambda i: (0, i)),
        ],
        out_specs=whole_spec((NG, rows)),
        out_shape=jax.ShapeDtypeStruct((NG, rows), jnp.float32),
        scratch_shapes=[
            pltpu.VMEM((rows, NG), jnp.float32),
            pltpu.VMEM((rows, chunk), jnp.bfloat16),
            pltpu.VMEM((rows, chunk), jnp.bfloat16),
        ],
        compiler_params=parallel,
        name="spread",
    )(first, basis_arr, own)

    def exchange(value):
        value = value.reshape(devices, share, rows)
        value = lax.all_to_all(value, MESH_AXES, split_axis=0, concat_axis=0, tiled=True)
        return value.reshape(NG, rows)

    received = exchange(charge)
    at = ((pen_at * groups + grp_at) * domains + dom_at) * share + lax.iota(jnp.int32, share)
    own_line = jnp.asarray(line.astype(np.float32))[at]
    own_sq = jnp.asarray((freq * freq).astype(np.float32))[at]
    returned = pl.pallas_call(
        lambda *refs: spectral_kernel(*refs, sizes=sizes),
        in_specs=[smem_spec(), smem_spec()] + [whole_spec((NG, NG))] * 5 + [whole_spec((NG, rows))],
        out_specs=whole_spec((NG, rows)),
        out_shape=jax.ShapeDtypeStruct((NG, rows), jnp.float32),
        scratch_shapes=[
            pltpu.VMEM((pencils * block, rows), jnp.float32),
            pltpu.VMEM((slab * block, NG), jnp.float32),
        ],
        grid=(),
        name="spectral",
    )(own_line, own_sq, basis_arr, jnp.asarray(mixed), jnp.asarray(mixed.T), plane, plane_sq, received)
    coefs = exchange(returned)

    nearby = neighbours(own, domains, pencils)
    steps = np.arange(9)
    dom_seen = dom_at + jnp.asarray(steps // 3 - 1)
    pen_seen = pen_at + jnp.asarray(steps % 3 - 1)
    wrap = jnp.stack([dom_seen // domains, pen_seen // pencils]).astype(jnp.float32)
    short_out = pl.pallas_call(
        lambda *refs: pair_kernel(
            *refs,
            factors=(2.0 * domains, 2.0 * pencils, 2.0 * domains),
            scale=2.0 / math.sqrt(atom_count / domains),
        ),
        in_specs=[smem_spec(), smem_spec(), smem_spec(), whole_spec(nearby.shape)],
        out_specs=whole_spec((3, atom_count)),
        out_shape=jax.ShapeDtypeStruct((3, atom_count), jnp.float32),
        grid=(),
        name="pairs",
    )(pair_home.reshape(-1), pair_other.reshape(-1), wrap, nearby)

    chunk = 256
    long_scale = -0.4 * NG / math.sqrt(NG * atom_count * devices)
    long_out = pl.pallas_call(
        lambda *refs: interpolate_kernel(*refs, sizes=sizes, scale=long_scale),
        grid=(atom_count // chunk,),
        in_specs=[
            smem_spec(),
            whole_spec((NG, NG)),
            whole_spec((NG, rows)),
            pl.BlockSpec((4, chunk), lambda i: (0, i)),
        ],
        out_specs=pl.BlockSpec((3, chunk), lambda i: (0, i)),
        out_shape=jax.ShapeDtypeStruct((3, atom_count), jnp.float32),
        scratch_shapes=[
            pltpu.VMEM((rows, 3 * NG), jnp.bfloat16),
            pltpu.VMEM((rows, 2 * chunk), jnp.float32),
        ],
        compiler_params=parallel,
        name="interpolate",
    )(first, basis_arr, coefs, own)
    return (short_out.reshape(3, 1, 1, atom_count), long_out.reshape(3, 1, 1, atom_count))


def solution(mesh):
    placed = (P(None, "grp", "dom", "pen"), P("grp", "dom", "pen"), P("grp", "dom", "pen"))

    def body(atoms, pair_home, pair_other):
        sizes = fast_sizes(
            mesh.shape["grp"], mesh.shape["dom"], mesh.shape["pen"], atoms.shape[3]
        )
        if sizes is None:
            return on_device(atoms, pair_home, pair_other)
        return fast_on_device(atoms, pair_home, pair_other, sizes=sizes)

    return jax.shard_map(
        body,
        mesh=mesh,
        in_specs=placed,
        out_specs=(P(None, "grp", "dom", "pen"), P(None, "grp", "dom", "pen")),
        check_vma=False,
    )
```

```python
import math

import jax
import jax.numpy as jnp
import numpy as np
from jax import lax
from jax.experimental import pallas as pl
from jax.experimental.pallas import tpu as pltpu
from jax.sharding import PartitionSpec as P

NG = 128
TILE = 128


exact_precision = lax.Precision.HIGHEST


def with_halo(block, sides, width):
    for axis, dim in sides:
        count = lax.axis_size(axis)
        forward = [(i, i + 1) for i in range(count - 1)]
        forward.append((count - 1, 0))
        backward = [(target, source) for source, target in forward]
        low = lax.ppermute(
            lax.slice_in_dim(block, block.shape[dim] - width, None, axis=dim), axis, forward
        )
        high = lax.ppermute(lax.slice_in_dim(block, 0, width, axis=dim), axis, backward)
        block = jnp.concatenate([low, block, high], axis=dim)
    return block


def passed_along(block, axis, distance):
    devices = range(lax.axis_size(axis))
    route = [((i - distance) % len(devices), i) for i in devices]
    return lax.ppermute(block, axis, route)


def matmul(left, right):
    return jnp.dot(left, right, precision=exact_precision, preferred_element_type=jnp.float32)


def spline_terms(scaled):
    floored = jnp.floor(scaled)
    fraction = scaled - floored
    remain = 1.0 - fraction
    frac_sq = fraction * fraction
    frac_cube = frac_sq * fraction
    thetas = [
        remain * remain * remain / 6.0,
        (3.0 * frac_cube - 6.0 * frac_sq + 4.0) / 6.0,
        (-3.0 * frac_cube + 3.0 * frac_sq + 3.0 * fraction + 1.0) / 6.0,
        frac_cube / 6.0,
    ]
    slopes = [
        -0.5 * remain * remain,
        1.5 * frac_sq - 2.0 * fraction,
        -1.5 * frac_sq + fraction + 0.5,
        0.5 * frac_sq,
    ]
    return (floored.astype(jnp.int32) - 3, thetas, slopes)


def spline_rows(coords, anchor, planes, grid_cells):
    lowest, thetas, slopes = spline_terms(coords * grid_cells)
    plane_ids = lax.broadcasted_iota(jnp.int32, (planes, 1), 0)
    values = jnp.zeros((planes, coords.shape[0]), jnp.float32)
    slopes_out = jnp.zeros_like(values)
    for offset in range(4):
        matches = (jnp.mod(lowest + offset - anchor, grid_cells)[None, :] == plane_ids).astype(
            jnp.float32
        )
        values = values + matches * thetas[offset][None, :]
        slopes_out = slopes_out + matches * slopes[offset][None, :]
    return (values, slopes_out)


def pair_push(home_pos, other_pos, scales):
    displace = home_pos[:, :3, :, None] - other_pos[:, :3, None, :]
    displace = displace - jnp.floor(displace + 0.5)
    scaled = displace * scales[None, :, None, None]
    weight = jnp.exp(-0.5 * jnp.sum(scaled * scaled, axis=1)) * other_pos[:, 3, None, :]
    return jnp.sum(scaled * weight[:, None], axis=3) * home_pos[:, 3:4, :]


def green_factor(freq_x, freq_y, freq_z, grid_cells):

    def signed(frequencies):
        return jnp.where(frequencies < grid_cells // 2, frequencies, frequencies - grid_cells)

    def modulus(frequencies):
        turned = 2.0 * jnp.pi * signed(frequencies).astype(jnp.float32) / grid_cells
        ratio = (2.0 + jnp.cos(turned)) / 3.0
        return 1.0 / (ratio * ratio)

    signed_x = signed(freq_x)
    signed_y = signed(freq_y)
    signed_z = signed(freq_z)
    square = (signed_x * signed_x + signed_y * signed_y + signed_z * signed_z).astype(jnp.float32)
    beta = 0.6 * grid_cells
    safe = jnp.maximum(square, 1.0)
    value = jnp.exp(-jnp.pi * jnp.pi * square / (beta * beta)) / (jnp.pi * safe)
    value = value * modulus(freq_x) * modulus(freq_y) * modulus(freq_z)
    return jnp.where(square > 0.5, value, 0.0)


def phase_tables(frequencies, cell_ids, grid_cells):
    turns = jnp.mod(frequencies[:, None] * cell_ids[None, :], grid_cells).astype(jnp.float32)
    angle = turns * (2.0 * jnp.pi / grid_cells)
    return (jnp.cos(angle), jnp.sin(angle))


def spread_mesh(spread_atoms, first_x, first_y, slab_cells, column, grid_cells):
    span_size = min(1024, spread_atoms.shape[1])
    batches = spread_atoms.reshape(4, -1, span_size).transpose(1, 0, 2)

    def spread_step(totals, atom_batch):
        weight_x, _ = spline_rows(atom_batch[0], first_x, slab_cells, grid_cells)
        weight_y, _ = spline_rows(atom_batch[1], first_y, column, grid_cells)
        weight_z, _ = spline_rows(atom_batch[2], 0, grid_cells, grid_cells)
        weighted_y = weight_y * atom_batch[3][None, :]
        paired = weight_x[:, None, :] * weighted_y[None, :, :]
        paired = paired.reshape(slab_cells * column, span_size)
        product = lax.dot_general(
            paired,
            weight_z,
            (((1,), (1,)), ((), ())),
            precision=exact_precision,
            preferred_element_type=jnp.float32,
        )
        return (totals + product, None)

    totals, _ = lax.scan(
        spread_step, jnp.zeros((slab_cells * column, grid_cells), jnp.float32), batches
    )
    return totals


def forward_lines(cos_tab, sin_tab, real_part, imag_part):
    return (
        matmul(cos_tab, real_part) + matmul(sin_tab, imag_part),
        matmul(cos_tab, imag_part) - matmul(sin_tab, real_part),
    )


def inverse_lines(cos_tab, sin_tab, real_part, imag_part):
    return (
        matmul(cos_tab, real_part) - matmul(sin_tab, imag_part),
        matmul(cos_tab, imag_part) + matmul(sin_tab, real_part),
    )


def on_device(atoms, pair_home, pair_other):
    grid_cells = NG
    groups = lax.axis_size("grp")
    domains = lax.axis_size("dom")
    pencils = lax.axis_size("pen")
    slab_cells = grid_cells // domains
    column = grid_cells // pencils
    atom_count = atoms.shape[3]
    tile_count = atom_count // TILE
    dom_at = lax.axis_index("dom")
    pen_at = lax.axis_index("pen")
    grp_at = lax.axis_index("grp")
    first_x = dom_at * slab_cells
    first_y = pen_at * column
    local_atoms = atoms.reshape(1, 1, 4 * atom_count)
    nearby = with_halo(local_atoms, (("dom", 0), ("pen", 1)), 1)
    nearby = nearby.reshape(3, 3, 4, atom_count)
    tiled = (
        nearby.reshape(9, 4, tile_count, TILE)
        .transpose(0, 2, 1, 3)
        .reshape(9 * tile_count, 4, TILE)
    )
    own_tiles = tiled[4 * tile_count : 5 * tile_count]
    home_ids = pair_home.reshape(-1)
    other_ids = pair_other.reshape(-1)
    pair_count = home_ids.shape[0]
    scales = jnp.array([2.0 * domains, 2.0 * pencils, 2.0 * domains], jnp.float32)

    def pair_group(id_pair):
        home_blk, other_blk = id_pair
        return pair_push(own_tiles[home_blk], tiled[other_blk], scales)

    pushes = lax.map(pair_group, (home_ids.reshape(-1, 16), other_ids.reshape(-1, 16)))
    pushes = pushes.reshape(pair_count, 3 * TILE)
    owners = (home_ids[:, None] == lax.broadcasted_iota(jnp.int32, (1, tile_count), 1)).astype(
        jnp.float32
    )
    summed = lax.dot_general(
        owners,
        pushes,
        (((0,), (0,)), ((), ())),
        precision=exact_precision,
        preferred_element_type=jnp.float32,
    )
    short_out = summed.reshape(tile_count, 3, TILE).transpose(1, 0, 2).reshape(3, 1, 1, atom_count)
    short_out = short_out * (2.0 / math.sqrt(atom_count / domains))
    spread_atoms = nearby[1:3, 1:3].transpose(2, 0, 1, 3).reshape(4, 4 * atom_count)
    z_ids = lax.iota(jnp.int32, grid_cells)
    cos_z, sin_z = phase_tables(z_ids, z_ids, grid_cells)
    charge_mesh = spread_mesh(spread_atoms, first_x, first_y, slab_cells, column, grid_cells)
    kz_rows = grid_cells // groups
    kz_part = kz_rows // domains
    kx_part = grid_cells // pencils
    z_real = matmul(charge_mesh, cos_z)
    z_imag = -matmul(charge_mesh, sin_z)
    sum_real, sum_imag = (
        lax.psum_scatter(z_real, "grp", scatter_dimension=1, tiled=True),
        lax.psum_scatter(z_imag, "grp", scatter_dimension=1, tiled=True),
    )
    sum_real = sum_real.reshape(slab_cells, column, kz_rows)
    sum_imag = sum_imag.reshape(slab_cells, column, kz_rows)
    line_real, line_imag = (
        lax.all_to_all(sum_real, "dom", split_axis=2, concat_axis=0, tiled=True),
        lax.all_to_all(sum_imag, "dom", split_axis=2, concat_axis=0, tiled=True),
    )
    fx_real, fx_imag = forward_lines(
        cos_z,
        sin_z,
        line_real.reshape(grid_cells, column * kz_part),
        line_imag.reshape(grid_cells, column * kz_part),
    )
    fx_real = fx_real.reshape(grid_cells, column, kz_part)
    fx_imag = fx_imag.reshape(grid_cells, column, kz_part)
    ylin_real, ylin_imag = (
        lax.all_to_all(fx_real, "pen", split_axis=0, concat_axis=1, tiled=True),
        lax.all_to_all(fx_imag, "pen", split_axis=0, concat_axis=1, tiled=True),
    )
    ylin_real = ylin_real.transpose(1, 0, 2).reshape(grid_cells, kx_part * kz_part)
    ylin_imag = ylin_imag.transpose(1, 0, 2).reshape(grid_cells, kx_part * kz_part)
    fy_real, fy_imag = forward_lines(cos_z, sin_z, ylin_real, ylin_imag)
    kx_ids = pen_at * kx_part + lax.iota(jnp.int32, kx_part)
    kz_ids = grp_at * kz_rows + dom_at * kz_part + lax.iota(jnp.int32, kz_part)
    factor = green_factor(
        kx_ids[None, :, None], z_ids[:, None, None], kz_ids[None, None, :], grid_cells
    )
    factor = factor.reshape(grid_cells, kx_part * kz_part)
    iy_real, iy_imag = inverse_lines(cos_z, sin_z, fy_real * factor, fy_imag * factor)
    iy_real = iy_real.reshape(grid_cells, kx_part, kz_part).transpose(1, 0, 2)
    iy_imag = iy_imag.reshape(grid_cells, kx_part, kz_part).transpose(1, 0, 2)
    back_real, back_imag = (
        lax.all_to_all(iy_real, "pen", split_axis=1, concat_axis=0, tiled=True),
        lax.all_to_all(iy_imag, "pen", split_axis=1, concat_axis=0, tiled=True),
    )
    ix_real, ix_imag = inverse_lines(
        cos_z,
        sin_z,
        back_real.reshape(grid_cells, column * kz_part),
        back_imag.reshape(grid_cells, column * kz_part),
    )
    ix_real = ix_real.reshape(grid_cells, column, kz_part)
    ix_imag = ix_imag.reshape(grid_cells, column, kz_part)
    slab_real, slab_imag = (
        lax.all_to_all(ix_real, "dom", split_axis=0, concat_axis=2, tiled=True),
        lax.all_to_all(ix_imag, "dom", split_axis=0, concat_axis=2, tiled=True),
    )
    whole_real, whole_imag = (
        lax.all_gather(slab_real, "grp", axis=2, tiled=True),
        lax.all_gather(slab_imag, "grp", axis=2, tiled=True),
    )
    own_pot = matmul(whole_real.reshape(-1, grid_cells), cos_z) - matmul(
        whole_imag.reshape(-1, grid_cells), sin_z
    )
    own_pot = own_pot.reshape(slab_cells, column, grid_cells)
    lower_planes = passed_along(own_pot[slab_cells - 3 :], "dom", 1)
    taller = jnp.concatenate([lower_planes, own_pot], axis=0)
    side_planes = passed_along(taller[:, column - 3 :], "pen", 1)
    rimmed = jnp.concatenate([side_planes, taller], axis=1)
    flat_pot = rimmed.transpose(1, 0, 2).reshape(-1, grid_cells)
    batch_size = min(256, atom_count)
    own_atoms = atoms.reshape(4, -1, batch_size).transpose(1, 0, 2)

    def interpolate(atom_batch):
        weight_x, slope_x = spline_rows(atom_batch[0], first_x - 3, slab_cells + 3, grid_cells)
        weight_y, slope_y = spline_rows(atom_batch[1], first_y - 3, column + 3, grid_cells)
        weight_z, slope_zw = spline_rows(atom_batch[2], 0, grid_cells, grid_cells)
        along_z = matmul(flat_pot, weight_z).reshape(column + 3, slab_cells + 3, batch_size)
        slope_z = matmul(flat_pot, slope_zw).reshape(column + 3, slab_cells + 3, batch_size)
        grad_x = jnp.sum(weight_y[:, None] * slope_x[None] * along_z, axis=(0, 1))
        grad_y = jnp.sum(slope_y[:, None] * weight_x[None] * along_z, axis=(0, 1))
        grad_z = jnp.sum(weight_y[:, None] * weight_x[None] * slope_z, axis=(0, 1))
        return jnp.stack([grad_x, grad_y, grad_z]) * atom_batch[3][None, :]

    gradients = lax.map(interpolate, own_atoms)
    gradients = gradients.transpose(1, 0, 2).reshape(3, 1, 1, atom_count)
    total_atoms = atom_count * groups * domains * pencils
    long_scale = -0.4 * grid_cells / math.sqrt(grid_cells * total_atoms)
    return (short_out, gradients * long_scale)


LANES = 128
SUBLANES = 8
MESH_AXES = ("pen", "grp", "dom")


def fast_sizes(groups, domains, pencils, atom_count):
    devices = groups * domains * pencils
    if NG != LANES or NG % devices or NG // domains != 32 or NG // pencils != 32:
        return None
    share = NG // devices
    if min(domains, pencils) < 4:
        return None
    if (domains * share) % SUBLANES or atom_count % 1024 or TILE != LANES:
        return None
    slab = NG // domains
    column = NG // pencils
    return dict(
        share=share,
        slab=slab,
        stride=column + 4,
        column=column,
        rows=-(-(slab + 3) * (column + 4) // LANES) * LANES,
        block=domains * share,
        groups=groups,
        domains=domains,
        pencils=pencils,
    )


def real_basis():
    freq = np.arange(NG)
    freq = np.where(freq <= NG // 2, freq, freq - NG // 2)
    turns = (freq[:, None] * np.arange(NG)[None, :]) % NG
    angle = turns * (2.0 * np.pi / NG)
    use_cos = (np.arange(NG) <= NG // 2)[:, None]
    return freq, np.where(use_cos, np.cos(angle), np.sin(angle)).astype(np.float32)


def line_factor(freq):
    beta = 0.6 * NG
    ratio = (2.0 + np.cos(2.0 * np.pi * freq / NG)) / 3.0
    count = np.where((freq == 0) | (freq == NG // 2), 1.0, 2.0)
    return count * np.exp(-np.pi * np.pi * freq * freq / (beta * beta)) / (ratio * ratio)


def split_bf16(value):
    high = value.astype(jnp.bfloat16)
    low = (value - high.astype(jnp.float32)).astype(jnp.bfloat16)
    return high, low


def choose(place, options):
    out = jnp.where(place == 0.0, options[0], 0.0)
    for k in range(1, 4):
        out = jnp.where(place == float(k), options[k], out)
    return out


def row_ids(count, lanes):
    return lax.broadcasted_iota(jnp.int32, (count, lanes), 0).astype(jnp.float32)


def spline_parts(coord):
    scaled = coord * float(NG)
    floored = jnp.floor(scaled)
    fraction = scaled - floored
    remain = 1.0 - fraction
    frac_sq = fraction * fraction
    frac_cube = frac_sq * fraction
    sixth = 1.0 / 6.0
    thetas = [
        remain * remain * remain * sixth,
        (3.0 * frac_cube - 6.0 * frac_sq + 4.0) * sixth,
        (-3.0 * frac_cube + 3.0 * frac_sq + 3.0 * fraction + 1.0) * sixth,
        frac_cube * sixth,
    ]
    slopes = [
        -0.5 * remain * remain,
        1.5 * frac_sq - 2.0 * fraction,
        -1.5 * frac_sq + fraction + 0.5,
        0.5 * frac_sq,
    ]
    return floored, thetas, slopes


def z_place(floored, lanes):
    place = row_ids(NG, lanes) - floored + 3.0
    return jnp.where(place >= float(NG), place - float(NG), place)


def repeated_row(ref, table, row):
    return ref[table, pl.ds(row, SUBLANES, stride=0), :]


def period_ids(stride):
    period = row_ids(2 * stride, LANES)
    return jnp.where(period >= float(stride), period - float(stride), period)


def spread_kernel(
    place_ref, basis_ref, atoms_ref, out_ref, acc_ref, row_ref,
    high_a, low_a, z_a, high_b, low_b, z_b, *, sizes
):
    chunk_tiles = z_a.shape[1] // LANES
    chunks = atoms_ref.shape[1] // chunk_tiles
    rows, stride, share = sizes["rows"], sizes["stride"], sizes["share"]
    low_half = lax.broadcasted_iota(jnp.int32, (SUBLANES, LANES), 0) < stride % SUBLANES
    middle = stride // SUBLANES
    contract = (((1,), (1,)), ((), ()))

    def build(chunk, side, high_ref, low_ref, z_ref):
        for block in range(chunk_tiles):
            tile = chunk * chunk_tiles + block
            span = slice(block * LANES, (block + 1) * LANES)
            parts = [atoms_ref[part, pl.ds(tile, 1), :] for part in range(4)]
            floor_x, theta_x, _ = spline_parts(parts[0])
            floor_y, theta_y, _ = spline_parts(parts[1])
            floor_z, theta_z, _ = spline_parts(parts[2])
            floor_x = floor_x - place_ref[0].astype(jnp.float32)
            floor_y = floor_y - place_ref[1].astype(jnp.float32)
            z_high, z_low = split_bf16(choose(z_place(floor_z, LANES), theta_z))
            z_ref[:NG, span] = z_high
            z_ref[NG:, span] = z_low
            table = side * chunk_tiles + block
            row_ref[table, :, :] = choose(row_ids(stride + 4, LANES) - floor_x, theta_x)
            weight_y = choose(period_ids(stride) - floor_y, theta_y) * parts[3]
            for group in range(-(-rows // (4 * stride))):
                pieces = []
                for at in range(4 * group, min(4 * group + 4, sizes["slab"] + 4), 2):
                    first = repeated_row(row_ref, table, at)
                    second = repeated_row(row_ref, table, at + 1)
                    mixed = jnp.where(low_half, first, second)
                    for step in range(2 * stride // SUBLANES):
                        factor = first if step < middle else mixed if step == middle else second
                        pieces.append(factor * weight_y[step * SUBLANES : (step + 1) * SUBLANES, :])
                start = group * 4 * stride
                count = min(4 * stride, rows - start)
                high, low = split_bf16(jnp.concatenate(pieces[: count // SUBLANES], axis=0))
                high_ref[start : start + count, span] = high
                low_ref[start : start + count, span] = low

    def add(high_ref, low_ref, z_ref):
        main = lax.dot_general(
            high_ref[...], z_ref[...], contract, preferred_element_type=jnp.float32
        )
        rest = lax.dot_general(
            low_ref[...], z_ref[:NG, :], contract, preferred_element_type=jnp.float32
        )
        acc_ref[:, : 2 * NG] += main
        acc_ref[:, 2 * NG :] += rest

    acc_ref[...] = jnp.zeros_like(acc_ref)
    set_a, set_b = (high_a, low_a, z_a), (high_b, low_b, z_b)
    build(0, 0, *set_a)

    def two_chunks(step, carry):
        build(2 * step + 1, 1, *set_b)
        add(*set_a)
        build(2 * step + 2, 0, *set_a)
        add(*set_b)
        return carry

    lax.fori_loop(0, chunks // 2 - 1, two_chunks, 0)
    build(chunks - 1, 1, *set_b)
    add(*set_a)
    add(*set_b)
    result = lax.dot_general(
        basis_ref[...],
        acc_ref[:, :NG] + acc_ref[:, NG : 2 * NG] + acc_ref[:, 2 * NG :],
        contract,
        precision=exact_precision,
        preferred_element_type=jnp.float32,
    )
    for target in range(NG // share):
        out_ref[target, :, :] = result[target * share : (target + 1) * share, :]


def ring_mask(lane, start, length):
    start = start % LANES
    if start + length <= LANES:
        return (lane >= start) & (lane < start + length)
    return (lane >= start) | (lane < start + length - LANES)


def spectral_kernel(
    place_ref, line_ref, basis_ref, mixed_ref, mixed_t_ref, plane_ref, plane_sq_ref,
    in_ref, out_ref, sum_ref, work_ref, *, sizes
):
    block, share, stride = sizes["block"], sizes["share"], sizes["stride"]
    slab, column, groups = sizes["slab"], sizes["column"], sizes["groups"]
    pencils, rows = sizes["pencils"], sizes["rows"]
    domains = sizes["domains"]
    for pen in range(pencils):
        pieces = []
        for dom in range(domains):
            total = in_ref[pen * groups * domains + dom, :, :]
            for grp in range(1, groups):
                total = total + in_ref[(pen * groups + grp) * domains + dom, :, :]
            pieces.append(total)
        sum_ref[pen * block : (pen + 1) * block, :] = jnp.concatenate(pieces, axis=0)
    lane = lax.broadcasted_iota(jnp.int32, (block, LANES), 1)
    width = column + 3

    def gathered(x):
        total = None
        for pen in range(pencils):
            shift = (column * pen - 3 - stride * x) % LANES
            for tile in range(stride * x // LANES, (stride * x + width - 1) // LANES + 1):
                low = max(0, tile * LANES - stride * x)
                high = min(width, (tile + 1) * LANES - stride * x)
                part = sum_ref[pen * block : (pen + 1) * block, tile * LANES : (tile + 1) * LANES]
                part = pltpu.roll(part, shift, 1) if shift else part
                mask = ring_mask(lane, column * pen - 3 + low, high - low)
                part = jnp.where(mask, part, 0.0)
                total = part if total is None else total + part
        return total

    for x in range(slab):
        value = gathered(x + 3)
        if x >= slab - 3:
            value = value + pltpu.roll(gathered(x + 3 - slab), block - share, 0)
        work_ref[x * block : (x + 1) * block, :] = value

    def dot(left, right, contract=(1, 0)):
        return lax.dot_general(
            left,
            right,
            (((contract[0],), (contract[1],)), ((), ())),
            precision=exact_precision,
            preferred_element_type=jnp.float32,
        )

    work_ref[...] = dot(work_ref[...], basis_ref[...], (1, 1))
    for kz in range(share):
        picked = work_ref[pl.ds(kz, NG, stride=share), :]
        spectrum = dot(mixed_ref[...], picked)
        at = place_ref[2] + kz
        freq = jnp.where(at > NG // 2, at - NG // 2, at)
        square = plane_sq_ref[...] + (freq * freq).astype(jnp.float32)
        factor = plane_ref[...] * line_ref[freq] / jnp.maximum(square, 1.0)
        factor = jnp.where(square > 0.5, factor, 0.0)
        work_ref[pl.ds(kz, NG, stride=share), :] = dot(mixed_t_ref[...], spectrum * factor)
    work_ref[...] = dot(work_ref[...], basis_ref[...])

    for pen in range(pencils):
        for tile in range(rows // LANES):
            total = jnp.zeros((block, LANES), jnp.float32)
            for x in range(slab + 3):
                low = max(stride * x, tile * LANES)
                high = min(stride * x + width, (tile + 1) * LANES)
                if low >= high:
                    continue
                if x >= 3:
                    value = work_ref[(x - 3) * block : (x - 2) * block, :]
                else:
                    value = work_ref[(slab - 3 + x) * block : (slab - 2 + x) * block, :]
                    value = pltpu.roll(value, share, 0)
                shift = (stride * x - column * pen + 3) % LANES
                value = pltpu.roll(value, shift, 1) if shift else value
                mask = ring_mask(lane, low - tile * LANES, high - low)
                total = jnp.where(mask, value, total)
            span = slice(tile * LANES, (tile + 1) * LANES)
            for dom in range(domains):
                part = total[dom * share : (dom + 1) * share, :]
                for grp in range(groups):
                    out_ref[(pen * groups + grp) * domains + dom, :, span] = part


def interpolate_kernel(
    place_ref, basis_ref, coef_ref, atoms_ref, out_ref, pot_ref, table_ref,
    along_a, weight_a, along_b, weight_b, *, sizes, scale
):
    lanes = along_a.shape[1] // 2
    tiles = lanes // LANES
    chunks = atoms_ref.shape[1] // tiles
    rows, stride = sizes["rows"], sizes["stride"]
    coefs = jnp.concatenate([coef_ref[source, :, :] for source in range(coef_ref.shape[0])], axis=0)
    high, low = split_bf16(coefs)
    basis_high, basis_low = split_bf16(basis_ref[...])
    potential = lax.dot_general(
        jnp.concatenate([high, low, high], axis=0),
        jnp.concatenate([basis_high, basis_high, basis_low], axis=0),
        (((0,), (0,)), ((), ())),
        preferred_element_type=jnp.float32,
    )
    high, low = split_bf16(potential)
    pot_ref[:, :NG] = high
    pot_ref[:, NG : 2 * NG] = low
    pot_ref[:, 2 * NG :] = high
    low_half = lax.broadcasted_iota(jnp.int32, (SUBLANES, LANES), 0) < stride % SUBLANES
    middle = stride // SUBLANES

    def contract_z(chunk, along_ref, weight_ref):
        for block in range(tiles):
            tile = chunk * tiles + block
            floor_z, theta_z, slope_z = spline_parts(atoms_ref[2, pl.ds(tile, 1), :])
            place = z_place(floor_z, LANES)
            for kind, options in enumerate((theta_z, slope_z)):
                span = slice(kind * lanes + block * LANES, kind * lanes + (block + 1) * LANES)
                high, low = split_bf16(choose(place, options))
                weight_ref[:NG, span] = high
                weight_ref[NG : 2 * NG, span] = high
                weight_ref[2 * NG :, span] = low
        along_ref[...] = jnp.dot(
            pot_ref[...], weight_ref[...], preferred_element_type=jnp.float32
        )

    def finish(chunk, side, along_ref):
        for block in range(tiles):
            tile = chunk * tiles + block
            parts = [atoms_ref[part, pl.ds(tile, 1), :] for part in (0, 1, 3)]
            floor_x, theta_x, slope_x = spline_parts(parts[0])
            floor_y, theta_y, slope_y = spline_parts(parts[1])
            floor_x = floor_x - place_ref[0].astype(jnp.float32)
            floor_y = floor_y - place_ref[1].astype(jnp.float32)
            place = row_ids(stride + 4, LANES) - floor_x
            kept = 2 * (side * tiles + block)
            table_ref[kept, :, :] = choose(place, theta_x)
            table_ref[kept + 1, :, :] = choose(place, slope_x)
            place = period_ids(stride) - floor_y
            weight_y, deriv_y = choose(place, theta_y), choose(place, slope_y)
            grads = [jnp.zeros((SUBLANES, LANES), jnp.float32) for _ in range(3)]
            for at in range(0, sizes["slab"] + 3, 2):
                sums = [[None] * 3 for _ in range(3)]
                for step in range(2 * stride // SUBLANES):
                    row = at * stride + step * SUBLANES
                    if row >= rows:
                        continue
                    here = slice(row, row + SUBLANES)
                    span = slice(step * SUBLANES, (step + 1) * SUBLANES)
                    along = along_ref[here, block * LANES : (block + 1) * LANES]
                    slope = along_ref[here, lanes + block * LANES : lanes + (block + 1) * LANES]
                    kind = 0 if step < middle else 1 if step == middle else 2
                    terms = (along * weight_y[span], along * deriv_y[span], slope * weight_y[span])
                    for axis in range(3):
                        held = sums[axis][kind]
                        sums[axis][kind] = terms[axis] if held is None else held + terms[axis]
                factors = []
                for table in range(2):
                    first = repeated_row(table_ref, kept + table, at)
                    second = repeated_row(table_ref, kept + table, at + 1)
                    factors.append((first, jnp.where(low_half, first, second), second))
                for axis, table in enumerate((1, 0, 0)):
                    for kind in range(3):
                        grads[axis] = grads[axis] + sums[axis][kind] * factors[table][kind]
            charge = parts[2] * scale
            for axis in range(3):
                row = jnp.sum(grads[axis], axis=0, keepdims=True) * charge
                out_ref[axis, pl.ds(tile, 1), :] = row

    set_a, set_b = (along_a, weight_a), (along_b, weight_b)
    contract_z(0, *set_a)

    def two_chunks(step, carry):
        contract_z(2 * step + 1, *set_b)
        finish(2 * step, 0, along_a)
        contract_z(2 * step + 2, *set_a)
        finish(2 * step + 1, 1, along_b)
        return carry

    lax.fori_loop(0, chunks // 2 - 1, two_chunks, 0)
    contract_z(chunks - 1, *set_b)
    finish(chunks - 2, 0, along_a)
    finish(chunks - 1, 1, along_b)


def pair_kernel(
    home_ref, other_ref, place_ref, near_ref, out_ref, *, factors, scale, domains, pencils, together
):
    tiles = near_ref.shape[2]
    out_ref[...] = jnp.zeros_like(out_ref)

    def wrapped(seen, count):
        return jnp.where(seen < 0, -1.0, jnp.where(seen >= count, 1.0, 0.0))

    def one_pair(n):
        home = home_ref[n]
        other = other_ref[n]
        around = other // tiles
        tile = other - around * tiles
        step_dom = around // 3
        wrap_x = wrapped(place_ref[3] + step_dom - 1, domains)
        wrap_y = wrapped(place_ref[4] + around - 3 * step_dom - 1, pencils)
        mine = [near_ref[4, part, pl.ds(home, 1), :] for part in range(4)]
        theirs = jnp.concatenate(
            [near_ref[around, part, pl.ds(tile, 1), :] for part in range(4)] * 2, axis=0
        ).T
        delta_x = (mine[0] - wrap_x) - theirs[:, 0:1]
        delta_y = (mine[1] - wrap_y) - theirs[:, 1:2]
        delta_z = mine[2] - theirs[:, 2:3]
        delta_z = delta_z - jnp.floor(delta_z + 0.5)
        scaled = (delta_x * factors[0], delta_y * factors[1], delta_z * factors[2])
        square = scaled[0] * scaled[0] + scaled[1] * scaled[1] + scaled[2] * scaled[2]
        weight = jnp.exp(-0.5 * square) * theirs[:, 3:4]
        charge = mine[3] * scale
        return home, [jnp.sum(part * weight, axis=0, keepdims=True) * charge for part in scaled]

    def some_pairs(step, carry):
        found = [one_pair(step * together + n) for n in range(together)]
        for home, pushes in found:
            for axis in range(3):
                out_ref[axis, pl.ds(home, 1), :] += pushes[axis]
        return carry

    lax.fori_loop(0, home_ref.shape[0] // together, some_pairs, 0)


def neighbours(block):
    near = block[None]
    for axis in ("pen", "dom"):
        count = lax.axis_size(axis)
        up = [(i, (i + 1) % count) for i in range(count)]
        down = [(i, (i - 1) % count) for i in range(count)]
        lower = lax.ppermute(near, axis, up)
        upper = lax.ppermute(near, axis, down)
        near = jnp.concatenate([lower, near, upper], axis=0)
    return near


def in_vmem(value):
    return pltpu.with_memory_space_constraint(jnp.asarray(value), pltpu.VMEM)


def whole_spec():
    return pl.BlockSpec(memory_space=pltpu.VMEM)


def smem_spec():
    return pl.BlockSpec(memory_space=pltpu.SMEM)


def fast_on_device(atoms, pair_home, pair_other, *, sizes):
    groups, domains, pencils = sizes["groups"], sizes["domains"], sizes["pencils"]
    rows, share, block = sizes["rows"], sizes["share"], sizes["block"]
    slab, column, stride = sizes["slab"], sizes["column"], sizes["stride"]
    devices = groups * domains * pencils
    atom_count = atoms.shape[3]
    tiles = atom_count // LANES
    own = atoms.reshape(4, tiles, LANES)
    dom_at = lax.axis_index("dom")
    pen_at = lax.axis_index("pen")
    grp_at = lax.axis_index("grp")
    line_at = ((pen_at * groups + grp_at) * domains + dom_at) * share
    place = jnp.stack([dom_at * slab, pen_at * column, line_at, dom_at, pen_at]).astype(jnp.int32)
    freq, basis = real_basis()
    order = (np.arange(domains)[None, :] * slab + np.arange(slab)[:, None]).reshape(-1)
    mixed = np.ascontiguousarray(basis[:, order])
    line = line_factor(freq)
    plane = in_vmem((line[:, None] * line[None, :] / np.pi).astype(np.float32))
    plane_sq = in_vmem((freq[:, None] ** 2 + freq[None, :] ** 2).astype(np.float32))
    basis_arr = jnp.asarray(basis)
    message = pltpu.VMEM((devices, share, rows), jnp.float32)

    nearby = in_vmem(neighbours(own))

    chunk = 512
    charge = pl.pallas_call(
        lambda *refs: spread_kernel(*refs, sizes=sizes),
        in_specs=[smem_spec(), whole_spec(), whole_spec()],
        out_specs=whole_spec(),
        out_shape=message,
        scratch_shapes=[
            pltpu.VMEM((rows, 3 * NG), jnp.float32),
            pltpu.VMEM((2 * chunk // LANES, stride + 4, LANES), jnp.float32),
        ]
        + [
            pltpu.VMEM((rows, chunk), jnp.bfloat16),
            pltpu.VMEM((rows, chunk), jnp.bfloat16),
            pltpu.VMEM((2 * NG, chunk), jnp.bfloat16),
        ]
        * 2,
        grid=(),
        name="spread",
    )(place, basis_arr, own)

    def exchange(value):
        value = lax.all_to_all(value, MESH_AXES, split_axis=0, concat_axis=0, tiled=True)
        return in_vmem(value)

    received = exchange(charge)
    returned = pl.pallas_call(
        lambda *refs: spectral_kernel(*refs, sizes=sizes),
        in_specs=[smem_spec(), smem_spec()]
        + [whole_spec()] * 5
        + [whole_spec()],
        out_specs=whole_spec(),
        out_shape=message,
        scratch_shapes=[
            pltpu.VMEM((pencils * block, rows), jnp.float32),
            pltpu.VMEM((slab * block, NG), jnp.float32),
        ],
        grid=(),
        name="spectral",
    )(
        place,
        jnp.asarray(line[: NG // 2 + 1].astype(np.float32)),
        basis_arr,
        in_vmem(mixed),
        in_vmem(mixed.T),
        plane,
        plane_sq,
        received,
    )
    coefs = exchange(returned)

    out_shape = jax.ShapeDtypeStruct((3, tiles, LANES), jnp.float32)
    pairs = pair_home.size
    short_out = pl.pallas_call(
        lambda *refs: pair_kernel(
            *refs,
            factors=(2.0 * domains, 2.0 * pencils, 2.0 * domains),
            scale=2.0 / math.sqrt(atom_count / domains),
            domains=domains,
            pencils=pencils,
            together=math.gcd(4, pairs),
        ),
        in_specs=[smem_spec(), smem_spec(), smem_spec(), whole_spec()],
        out_specs=whole_spec(),
        out_shape=out_shape,
        grid=(),
        name="pairs",
    )(pair_home.reshape(-1), pair_other.reshape(-1), place, nearby)

    chunk = 256
    long_scale = -0.4 * NG / math.sqrt(NG * atom_count * devices)
    long_out = pl.pallas_call(
        lambda *refs: interpolate_kernel(*refs, sizes=sizes, scale=long_scale),
        in_specs=[smem_spec(), whole_spec(), whole_spec(), whole_spec()],
        out_specs=whole_spec(),
        out_shape=out_shape,
        scratch_shapes=[
            pltpu.VMEM((rows, 3 * NG), jnp.bfloat16),
            pltpu.VMEM((4 * chunk // LANES, stride + 4, LANES), jnp.float32),
        ]
        + [
            pltpu.VMEM((rows, 2 * chunk), jnp.float32),
            pltpu.VMEM((3 * NG, 2 * chunk), jnp.bfloat16),
        ]
        * 2,
        grid=(),
        name="interpolate",
    )(place, basis_arr, coefs, own)
    return (short_out.reshape(3, 1, 1, atom_count), long_out.reshape(3, 1, 1, atom_count))


def solution(mesh):
    placed = (P(None, "grp", "dom", "pen"), P("grp", "dom", "pen"), P("grp", "dom", "pen"))

    def body(atoms, pair_home, pair_other):
        sizes = fast_sizes(
            mesh.shape["grp"], mesh.shape["dom"], mesh.shape["pen"], atoms.shape[3]
        )
        if sizes is None:
            return on_device(atoms, pair_home, pair_other)
        return fast_on_device(atoms, pair_home, pair_other, sizes=sizes)

    return jax.shard_map(
        body,
        mesh=mesh,
        in_specs=placed,
        out_specs=(P(None, "grp", "dom", "pen"), P(None, "grp", "dom", "pen")),
        check_vma=False,
    )
```

```python
import math

import jax
import jax.numpy as jnp
import numpy as np
from jax import lax
from jax.experimental import pallas as pl
from jax.experimental.pallas import tpu as pltpu
from jax.sharding import PartitionSpec as P

NG = 128
TILE = 128


exact_precision = lax.Precision.HIGHEST


def with_halo(block, sides, width):
    for axis, dim in sides:
        count = lax.axis_size(axis)
        forward = [(i, i + 1) for i in range(count - 1)]
        forward.append((count - 1, 0))
        backward = [(target, source) for source, target in forward]
        low = lax.ppermute(
            lax.slice_in_dim(block, block.shape[dim] - width, None, axis=dim), axis, forward
        )
        high = lax.ppermute(lax.slice_in_dim(block, 0, width, axis=dim), axis, backward)
        block = jnp.concatenate([low, block, high], axis=dim)
    return block


def passed_along(block, axis, distance):
    devices = range(lax.axis_size(axis))
    route = [((i - distance) % len(devices), i) for i in devices]
    return lax.ppermute(block, axis, route)


def matmul(left, right):
    return jnp.dot(left, right, precision=exact_precision, preferred_element_type=jnp.float32)


def spline_terms(scaled):
    floored = jnp.floor(scaled)
    fraction = scaled - floored
    remain = 1.0 - fraction
    frac_sq = fraction * fraction
    frac_cube = frac_sq * fraction
    thetas = [
        remain * remain * remain / 6.0,
        (3.0 * frac_cube - 6.0 * frac_sq + 4.0) / 6.0,
        (-3.0 * frac_cube + 3.0 * frac_sq + 3.0 * fraction + 1.0) / 6.0,
        frac_cube / 6.0,
    ]
    slopes = [
        -0.5 * remain * remain,
        1.5 * frac_sq - 2.0 * fraction,
        -1.5 * frac_sq + fraction + 0.5,
        0.5 * frac_sq,
    ]
    return (floored.astype(jnp.int32) - 3, thetas, slopes)


def spline_rows(coords, anchor, planes, grid_cells):
    lowest, thetas, slopes = spline_terms(coords * grid_cells)
    plane_ids = lax.broadcasted_iota(jnp.int32, (planes, 1), 0)
    values = jnp.zeros((planes, coords.shape[0]), jnp.float32)
    slopes_out = jnp.zeros_like(values)
    for offset in range(4):
        matches = (jnp.mod(lowest + offset - anchor, grid_cells)[None, :] == plane_ids).astype(
            jnp.float32
        )
        values = values + matches * thetas[offset][None, :]
        slopes_out = slopes_out + matches * slopes[offset][None, :]
    return (values, slopes_out)


def pair_push(home_pos, other_pos, scales):
    displace = home_pos[:, :3, :, None] - other_pos[:, :3, None, :]
    displace = displace - jnp.floor(displace + 0.5)
    scaled = displace * scales[None, :, None, None]
    weight = jnp.exp(-0.5 * jnp.sum(scaled * scaled, axis=1)) * other_pos[:, 3, None, :]
    return jnp.sum(scaled * weight[:, None], axis=3) * home_pos[:, 3:4, :]


def green_factor(freq_x, freq_y, freq_z, grid_cells):

    def signed(frequencies):
        return jnp.where(frequencies < grid_cells // 2, frequencies, frequencies - grid_cells)

    def modulus(frequencies):
        turned = 2.0 * jnp.pi * signed(frequencies).astype(jnp.float32) / grid_cells
        ratio = (2.0 + jnp.cos(turned)) / 3.0
        return 1.0 / (ratio * ratio)

    signed_x = signed(freq_x)
    signed_y = signed(freq_y)
    signed_z = signed(freq_z)
    square = (signed_x * signed_x + signed_y * signed_y + signed_z * signed_z).astype(jnp.float32)
    beta = 0.6 * grid_cells
    safe = jnp.maximum(square, 1.0)
    value = jnp.exp(-jnp.pi * jnp.pi * square / (beta * beta)) / (jnp.pi * safe)
    value = value * modulus(freq_x) * modulus(freq_y) * modulus(freq_z)
    return jnp.where(square > 0.5, value, 0.0)


def phase_tables(frequencies, cell_ids, grid_cells):
    turns = jnp.mod(frequencies[:, None] * cell_ids[None, :], grid_cells).astype(jnp.float32)
    angle = turns * (2.0 * jnp.pi / grid_cells)
    return (jnp.cos(angle), jnp.sin(angle))


def spread_mesh(spread_atoms, first_x, first_y, slab_cells, column, grid_cells):
    span_size = min(1024, spread_atoms.shape[1])
    batches = spread_atoms.reshape(4, -1, span_size).transpose(1, 0, 2)

    def spread_step(totals, atom_batch):
        weight_x, _ = spline_rows(atom_batch[0], first_x, slab_cells, grid_cells)
        weight_y, _ = spline_rows(atom_batch[1], first_y, column, grid_cells)
        weight_z, _ = spline_rows(atom_batch[2], 0, grid_cells, grid_cells)
        weighted_y = weight_y * atom_batch[3][None, :]
        paired = weight_x[:, None, :] * weighted_y[None, :, :]
        paired = paired.reshape(slab_cells * column, span_size)
        product = lax.dot_general(
            paired,
            weight_z,
            (((1,), (1,)), ((), ())),
            precision=exact_precision,
            preferred_element_type=jnp.float32,
        )
        return (totals + product, None)

    totals, _ = lax.scan(
        spread_step, jnp.zeros((slab_cells * column, grid_cells), jnp.float32), batches
    )
    return totals


def forward_lines(cos_tab, sin_tab, real_part, imag_part):
    return (
        matmul(cos_tab, real_part) + matmul(sin_tab, imag_part),
        matmul(cos_tab, imag_part) - matmul(sin_tab, real_part),
    )


def inverse_lines(cos_tab, sin_tab, real_part, imag_part):
    return (
        matmul(cos_tab, real_part) - matmul(sin_tab, imag_part),
        matmul(cos_tab, imag_part) + matmul(sin_tab, real_part),
    )


def on_device(atoms, pair_home, pair_other):
    grid_cells = NG
    groups = lax.axis_size("grp")
    domains = lax.axis_size("dom")
    pencils = lax.axis_size("pen")
    slab_cells = grid_cells // domains
    column = grid_cells // pencils
    atom_count = atoms.shape[3]
    tile_count = atom_count // TILE
    dom_at = lax.axis_index("dom")
    pen_at = lax.axis_index("pen")
    grp_at = lax.axis_index("grp")
    first_x = dom_at * slab_cells
    first_y = pen_at * column
    local_atoms = atoms.reshape(1, 1, 4 * atom_count)
    nearby = with_halo(local_atoms, (("dom", 0), ("pen", 1)), 1)
    nearby = nearby.reshape(3, 3, 4, atom_count)
    tiled = (
        nearby.reshape(9, 4, tile_count, TILE)
        .transpose(0, 2, 1, 3)
        .reshape(9 * tile_count, 4, TILE)
    )
    own_tiles = tiled[4 * tile_count : 5 * tile_count]
    home_ids = pair_home.reshape(-1)
    other_ids = pair_other.reshape(-1)
    pair_count = home_ids.shape[0]
    scales = jnp.array([2.0 * domains, 2.0 * pencils, 2.0 * domains], jnp.float32)

    def pair_group(id_pair):
        home_blk, other_blk = id_pair
        return pair_push(own_tiles[home_blk], tiled[other_blk], scales)

    pushes = lax.map(pair_group, (home_ids.reshape(-1, 16), other_ids.reshape(-1, 16)))
    pushes = pushes.reshape(pair_count, 3 * TILE)
    owners = (home_ids[:, None] == lax.broadcasted_iota(jnp.int32, (1, tile_count), 1)).astype(
        jnp.float32
    )
    summed = lax.dot_general(
        owners,
        pushes,
        (((0,), (0,)), ((), ())),
        precision=exact_precision,
        preferred_element_type=jnp.float32,
    )
    short_out = summed.reshape(tile_count, 3, TILE).transpose(1, 0, 2).reshape(3, 1, 1, atom_count)
    short_out = short_out * (2.0 / math.sqrt(atom_count / domains))
    spread_atoms = nearby[1:3, 1:3].transpose(2, 0, 1, 3).reshape(4, 4 * atom_count)
    z_ids = lax.iota(jnp.int32, grid_cells)
    cos_z, sin_z = phase_tables(z_ids, z_ids, grid_cells)
    charge_mesh = spread_mesh(spread_atoms, first_x, first_y, slab_cells, column, grid_cells)
    kz_rows = grid_cells // groups
    kz_part = kz_rows // domains
    kx_part = grid_cells // pencils
    z_real = matmul(charge_mesh, cos_z)
    z_imag = -matmul(charge_mesh, sin_z)
    sum_real, sum_imag = (
        lax.psum_scatter(z_real, "grp", scatter_dimension=1, tiled=True),
        lax.psum_scatter(z_imag, "grp", scatter_dimension=1, tiled=True),
    )
    sum_real = sum_real.reshape(slab_cells, column, kz_rows)
    sum_imag = sum_imag.reshape(slab_cells, column, kz_rows)
    line_real, line_imag = (
        lax.all_to_all(sum_real, "dom", split_axis=2, concat_axis=0, tiled=True),
        lax.all_to_all(sum_imag, "dom", split_axis=2, concat_axis=0, tiled=True),
    )
    fx_real, fx_imag = forward_lines(
        cos_z,
        sin_z,
        line_real.reshape(grid_cells, column * kz_part),
        line_imag.reshape(grid_cells, column * kz_part),
    )
    fx_real = fx_real.reshape(grid_cells, column, kz_part)
    fx_imag = fx_imag.reshape(grid_cells, column, kz_part)
    ylin_real, ylin_imag = (
        lax.all_to_all(fx_real, "pen", split_axis=0, concat_axis=1, tiled=True),
        lax.all_to_all(fx_imag, "pen", split_axis=0, concat_axis=1, tiled=True),
    )
    ylin_real = ylin_real.transpose(1, 0, 2).reshape(grid_cells, kx_part * kz_part)
    ylin_imag = ylin_imag.transpose(1, 0, 2).reshape(grid_cells, kx_part * kz_part)
    fy_real, fy_imag = forward_lines(cos_z, sin_z, ylin_real, ylin_imag)
    kx_ids = pen_at * kx_part + lax.iota(jnp.int32, kx_part)
    kz_ids = grp_at * kz_rows + dom_at * kz_part + lax.iota(jnp.int32, kz_part)
    factor = green_factor(
        kx_ids[None, :, None], z_ids[:, None, None], kz_ids[None, None, :], grid_cells
    )
    factor = factor.reshape(grid_cells, kx_part * kz_part)
    iy_real, iy_imag = inverse_lines(cos_z, sin_z, fy_real * factor, fy_imag * factor)
    iy_real = iy_real.reshape(grid_cells, kx_part, kz_part).transpose(1, 0, 2)
    iy_imag = iy_imag.reshape(grid_cells, kx_part, kz_part).transpose(1, 0, 2)
    back_real, back_imag = (
        lax.all_to_all(iy_real, "pen", split_axis=1, concat_axis=0, tiled=True),
        lax.all_to_all(iy_imag, "pen", split_axis=1, concat_axis=0, tiled=True),
    )
    ix_real, ix_imag = inverse_lines(
        cos_z,
        sin_z,
        back_real.reshape(grid_cells, column * kz_part),
        back_imag.reshape(grid_cells, column * kz_part),
    )
    ix_real = ix_real.reshape(grid_cells, column, kz_part)
    ix_imag = ix_imag.reshape(grid_cells, column, kz_part)
    slab_real, slab_imag = (
        lax.all_to_all(ix_real, "dom", split_axis=0, concat_axis=2, tiled=True),
        lax.all_to_all(ix_imag, "dom", split_axis=0, concat_axis=2, tiled=True),
    )
    whole_real, whole_imag = (
        lax.all_gather(slab_real, "grp", axis=2, tiled=True),
        lax.all_gather(slab_imag, "grp", axis=2, tiled=True),
    )
    own_pot = matmul(whole_real.reshape(-1, grid_cells), cos_z) - matmul(
        whole_imag.reshape(-1, grid_cells), sin_z
    )
    own_pot = own_pot.reshape(slab_cells, column, grid_cells)
    lower_planes = passed_along(own_pot[slab_cells - 3 :], "dom", 1)
    taller = jnp.concatenate([lower_planes, own_pot], axis=0)
    side_planes = passed_along(taller[:, column - 3 :], "pen", 1)
    rimmed = jnp.concatenate([side_planes, taller], axis=1)
    flat_pot = rimmed.transpose(1, 0, 2).reshape(-1, grid_cells)
    batch_size = min(256, atom_count)
    own_atoms = atoms.reshape(4, -1, batch_size).transpose(1, 0, 2)

    def interpolate(atom_batch):
        weight_x, slope_x = spline_rows(atom_batch[0], first_x - 3, slab_cells + 3, grid_cells)
        weight_y, slope_y = spline_rows(atom_batch[1], first_y - 3, column + 3, grid_cells)
        weight_z, slope_zw = spline_rows(atom_batch[2], 0, grid_cells, grid_cells)
        along_z = matmul(flat_pot, weight_z).reshape(column + 3, slab_cells + 3, batch_size)
        slope_z = matmul(flat_pot, slope_zw).reshape(column + 3, slab_cells + 3, batch_size)
        grad_x = jnp.sum(weight_y[:, None] * slope_x[None] * along_z, axis=(0, 1))
        grad_y = jnp.sum(slope_y[:, None] * weight_x[None] * along_z, axis=(0, 1))
        grad_z = jnp.sum(weight_y[:, None] * weight_x[None] * slope_z, axis=(0, 1))
        return jnp.stack([grad_x, grad_y, grad_z]) * atom_batch[3][None, :]

    gradients = lax.map(interpolate, own_atoms)
    gradients = gradients.transpose(1, 0, 2).reshape(3, 1, 1, atom_count)
    total_atoms = atom_count * groups * domains * pencils
    long_scale = -0.4 * grid_cells / math.sqrt(grid_cells * total_atoms)
    return (short_out, gradients * long_scale)


LANES = 128
SUBLANES = 8
MESH_AXES = ("pen", "grp", "dom")


def fast_sizes(groups, domains, pencils, atom_count):
    devices = groups * domains * pencils
    if NG != LANES or NG % devices or NG // domains != 32 or NG // pencils != 32:
        return None
    share = NG // devices
    if min(domains, pencils) < 4:
        return None
    if (domains * share) % SUBLANES or atom_count % 1024 or TILE != LANES:
        return None
    slab = NG // domains
    column = NG // pencils
    return dict(
        share=share,
        slab=slab,
        stride=column + 4,
        column=column,
        rows=-(-(slab + 3) * (column + 4) // LANES) * LANES,
        block=domains * share,
        groups=groups,
        domains=domains,
        pencils=pencils,
    )


def real_basis():
    freq = np.arange(NG)
    freq = np.where(freq <= NG // 2, freq, freq - NG // 2)
    turns = (freq[:, None] * np.arange(NG)[None, :]) % NG
    angle = turns * (2.0 * np.pi / NG)
    use_cos = (np.arange(NG) <= NG // 2)[:, None]
    return freq, np.where(use_cos, np.cos(angle), np.sin(angle)).astype(np.float32)


def line_factor(freq):
    beta = 0.6 * NG
    ratio = (2.0 + np.cos(2.0 * np.pi * freq / NG)) / 3.0
    count = np.where((freq == 0) | (freq == NG // 2), 1.0, 2.0)
    return count * np.exp(-np.pi * np.pi * freq * freq / (beta * beta)) / (ratio * ratio)


def split_bf16(value):
    high = value.astype(jnp.bfloat16)
    low = (value - high.astype(jnp.float32)).astype(jnp.bfloat16)
    return high, low


def choose(place, options):
    out = jnp.where(place == 0.0, options[0], 0.0)
    for k in range(1, 4):
        out = jnp.where(place == float(k), options[k], out)
    return out


def row_ids(count, lanes):
    return lax.broadcasted_iota(jnp.int32, (count, lanes), 0).astype(jnp.float32)


def spline_parts(coord):
    scaled = coord * float(NG)
    floored = jnp.floor(scaled)
    fraction = scaled - floored
    remain = 1.0 - fraction
    frac_sq = fraction * fraction
    frac_cube = frac_sq * fraction
    sixth = 1.0 / 6.0
    thetas = [
        remain * remain * remain * sixth,
        (3.0 * frac_cube - 6.0 * frac_sq + 4.0) * sixth,
        (-3.0 * frac_cube + 3.0 * frac_sq + 3.0 * fraction + 1.0) * sixth,
        frac_cube * sixth,
    ]
    slopes = [
        -0.5 * remain * remain,
        1.5 * frac_sq - 2.0 * fraction,
        -1.5 * frac_sq + fraction + 0.5,
        0.5 * frac_sq,
    ]
    return floored, thetas, slopes


def z_place(floored, lanes):
    place = row_ids(NG, lanes) - floored + 3.0
    return jnp.where(place >= float(NG), place - float(NG), place)


def repeated_row(ref, table, row):
    return ref[table, pl.ds(row, SUBLANES, stride=0), :]


def period_ids(stride):
    period = row_ids(2 * stride, LANES)
    return jnp.where(period >= float(stride), period - float(stride), period)


def spread_kernel(
    basis_ref, atoms_ref, out_ref, acc_ref, row_ref,
    high_a, low_a, z_a, high_b, low_b, z_b, *, sizes
):
    chunk_tiles = z_a.shape[1] // LANES
    chunks = atoms_ref.shape[1] // chunk_tiles
    rows, stride, share = sizes["rows"], sizes["stride"], sizes["share"]
    low_half = lax.broadcasted_iota(jnp.int32, (SUBLANES, LANES), 0) < stride % SUBLANES
    middle = stride // SUBLANES
    contract = (((1,), (1,)), ((), ()))

    def build(chunk, side, high_ref, low_ref, z_ref):
        for block in range(chunk_tiles):
            tile = chunk * chunk_tiles + block
            span = slice(block * LANES, (block + 1) * LANES)
            parts = [atoms_ref[part, pl.ds(tile, 1), :] for part in range(4)]
            floor_x, theta_x, _ = spline_parts(parts[0])
            floor_y, theta_y, _ = spline_parts(parts[1])
            floor_z, theta_z, _ = spline_parts(parts[2])
            floor_x = floor_x - (lax.axis_index("dom") * sizes["slab"]).astype(jnp.float32)
            floor_y = floor_y - (lax.axis_index("pen") * sizes["column"]).astype(jnp.float32)
            z_high, z_low = split_bf16(choose(z_place(floor_z, LANES), theta_z))
            z_ref[:NG, span] = z_high
            z_ref[NG:, span] = z_low
            table = side * chunk_tiles + block
            row_ref[table, :, :] = choose(row_ids(stride + 4, LANES) - floor_x, theta_x)
            weight_y = choose(period_ids(stride) - floor_y, theta_y) * parts[3]
            for group in range(-(-rows // (4 * stride))):
                pieces = []
                for at in range(4 * group, min(4 * group + 4, sizes["slab"] + 4), 2):
                    first = repeated_row(row_ref, table, at)
                    second = repeated_row(row_ref, table, at + 1)
                    mixed = jnp.where(low_half, first, second)
                    for step in range(2 * stride // SUBLANES):
                        factor = first if step < middle else mixed if step == middle else second
                        pieces.append(factor * weight_y[step * SUBLANES : (step + 1) * SUBLANES, :])
                start = group * 4 * stride
                count = min(4 * stride, rows - start)
                high, low = split_bf16(jnp.concatenate(pieces[: count // SUBLANES], axis=0))
                high_ref[start : start + count, span] = high
                low_ref[start : start + count, span] = low

    def add(high_ref, low_ref, z_ref):
        main = lax.dot_general(
            high_ref[...], z_ref[...], contract, preferred_element_type=jnp.float32
        )
        rest = lax.dot_general(
            low_ref[...], z_ref[:NG, :], contract, preferred_element_type=jnp.float32
        )
        acc_ref[:, : 2 * NG] += main
        acc_ref[:, 2 * NG :] += rest

    acc_ref[...] = jnp.zeros_like(acc_ref)
    set_a, set_b = (high_a, low_a, z_a), (high_b, low_b, z_b)
    build(0, 0, *set_a)

    def two_chunks(step, carry):
        build(2 * step + 1, 1, *set_b)
        add(*set_a)
        build(2 * step + 2, 0, *set_a)
        add(*set_b)
        return carry

    lax.fori_loop(0, chunks // 2 - 1, two_chunks, 0)
    build(chunks - 1, 1, *set_b)
    add(*set_a)
    add(*set_b)
    result = lax.dot_general(
        basis_ref[...],
        acc_ref[:, :NG] + acc_ref[:, NG : 2 * NG] + acc_ref[:, 2 * NG :],
        contract,
        precision=exact_precision,
        preferred_element_type=jnp.float32,
    )
    for target in range(NG // share):
        out_ref[target, :, :] = result[target * share : (target + 1) * share, :]


def ring_mask(lane, start, length):
    start = start % LANES
    if start + length <= LANES:
        return (lane >= start) & (lane < start + length)
    return (lane >= start) | (lane < start + length - LANES)


def spectral_kernel(
    line_ref, basis_ref, mixed_ref, mixed_t_ref, plane_ref, plane_sq_ref,
    in_ref, out_ref, sum_ref, work_ref, *, sizes
):
    block, share, stride = sizes["block"], sizes["share"], sizes["stride"]
    slab, column, groups = sizes["slab"], sizes["column"], sizes["groups"]
    pencils, rows = sizes["pencils"], sizes["rows"]
    domains = sizes["domains"]
    for pen in range(pencils):
        pieces = []
        for dom in range(domains):
            total = in_ref[pen * groups * domains + dom, :, :]
            for grp in range(1, groups):
                total = total + in_ref[(pen * groups + grp) * domains + dom, :, :]
            pieces.append(total)
        sum_ref[pen * block : (pen + 1) * block, :] = jnp.concatenate(pieces, axis=0)
    lane = lax.broadcasted_iota(jnp.int32, (block, LANES), 1)
    width = column + 3

    def gathered(x):
        total = None
        for pen in range(pencils):
            shift = (column * pen - 3 - stride * x) % LANES
            for tile in range(stride * x // LANES, (stride * x + width - 1) // LANES + 1):
                low = max(0, tile * LANES - stride * x)
                high = min(width, (tile + 1) * LANES - stride * x)
                part = sum_ref[pen * block : (pen + 1) * block, tile * LANES : (tile + 1) * LANES]
                part = pltpu.roll(part, shift, 1) if shift else part
                mask = ring_mask(lane, column * pen - 3 + low, high - low)
                part = jnp.where(mask, part, 0.0)
                total = part if total is None else total + part
        return total

    for x in range(slab):
        value = gathered(x + 3)
        if x >= slab - 3:
            value = value + pltpu.roll(gathered(x + 3 - slab), block - share, 0)
        work_ref[x * block : (x + 1) * block, :] = value

    def dot(left, right, contract=(1, 0)):
        return lax.dot_general(
            left,
            right,
            (((contract[0],), (contract[1],)), ((), ())),
            precision=exact_precision,
            preferred_element_type=jnp.float32,
        )

    work_ref[...] = dot(work_ref[...], basis_ref[...], (1, 1))
    device = (lax.axis_index("pen") * groups + lax.axis_index("grp")) * domains
    first_line = (device + lax.axis_index("dom")) * share
    for kz in range(share):
        picked = work_ref[pl.ds(kz, NG, stride=share), :]
        spectrum = dot(mixed_ref[...], picked)
        at = first_line + kz
        freq = jnp.where(at > NG // 2, at - NG // 2, at)
        square = plane_sq_ref[...] + (freq * freq).astype(jnp.float32)
        factor = plane_ref[...] * line_ref[pl.ds(freq, 1), :] / jnp.maximum(square, 1.0)
        factor = jnp.where(square > 0.5, factor, 0.0)
        work_ref[pl.ds(kz, NG, stride=share), :] = dot(mixed_t_ref[...], spectrum * factor)
    work_ref[...] = dot(work_ref[...], basis_ref[...])

    for pen in range(pencils):
        for tile in range(rows // LANES):
            total = jnp.zeros((block, LANES), jnp.float32)
            for x in range(slab + 3):
                low = max(stride * x, tile * LANES)
                high = min(stride * x + width, (tile + 1) * LANES)
                if low >= high:
                    continue
                if x >= 3:
                    value = work_ref[(x - 3) * block : (x - 2) * block, :]
                else:
                    value = work_ref[(slab - 3 + x) * block : (slab - 2 + x) * block, :]
                    value = pltpu.roll(value, share, 0)
                shift = (stride * x - column * pen + 3) % LANES
                value = pltpu.roll(value, shift, 1) if shift else value
                mask = ring_mask(lane, low - tile * LANES, high - low)
                total = jnp.where(mask, value, total)
            span = slice(tile * LANES, (tile + 1) * LANES)
            for dom in range(domains):
                part = total[dom * share : (dom + 1) * share, :]
                for grp in range(groups):
                    out_ref[(pen * groups + grp) * domains + dom, :, span] = part


def interpolate_kernel(
    basis_ref, coef_ref, atoms_ref, out_ref, pot_ref, table_ref,
    along_a, weight_a, along_b, weight_b, *, sizes, scale
):
    lanes = along_a.shape[1] // 2
    tiles = lanes // LANES
    chunks = atoms_ref.shape[1] // tiles
    rows, stride = sizes["rows"], sizes["stride"]
    coefs = jnp.concatenate([coef_ref[source, :, :] for source in range(coef_ref.shape[0])], axis=0)
    high, low = split_bf16(coefs)
    basis_high, basis_low = split_bf16(basis_ref[...])
    potential = lax.dot_general(
        jnp.concatenate([high, low, high], axis=0),
        jnp.concatenate([basis_high, basis_high, basis_low], axis=0),
        (((0,), (0,)), ((), ())),
        preferred_element_type=jnp.float32,
    )
    high, low = split_bf16(potential)
    pot_ref[:, :NG] = high
    pot_ref[:, NG : 2 * NG] = low
    pot_ref[:, 2 * NG :] = high
    low_half = lax.broadcasted_iota(jnp.int32, (SUBLANES, LANES), 0) < stride % SUBLANES
    middle = stride // SUBLANES

    def contract_z(chunk, along_ref, weight_ref):
        for block in range(tiles):
            tile = chunk * tiles + block
            floor_z, theta_z, slope_z = spline_parts(atoms_ref[2, pl.ds(tile, 1), :])
            place = z_place(floor_z, LANES)
            for kind, options in enumerate((theta_z, slope_z)):
                span = slice(kind * lanes + block * LANES, kind * lanes + (block + 1) * LANES)
                high, low = split_bf16(choose(place, options))
                weight_ref[:NG, span] = high
                weight_ref[NG : 2 * NG, span] = high
                weight_ref[2 * NG :, span] = low
        along_ref[...] = jnp.dot(
            pot_ref[...], weight_ref[...], preferred_element_type=jnp.float32
        )

    def finish(chunk, side, along_ref):
        for block in range(tiles):
            tile = chunk * tiles + block
            parts = [atoms_ref[part, pl.ds(tile, 1), :] for part in (0, 1, 3)]
            floor_x, theta_x, slope_x = spline_parts(parts[0])
            floor_y, theta_y, slope_y = spline_parts(parts[1])
            floor_x = floor_x - (lax.axis_index("dom") * sizes["slab"]).astype(jnp.float32)
            floor_y = floor_y - (lax.axis_index("pen") * sizes["column"]).astype(jnp.float32)
            place = row_ids(stride + 4, LANES) - floor_x
            kept = 2 * (side * tiles + block)
            table_ref[kept, :, :] = choose(place, theta_x)
            table_ref[kept + 1, :, :] = choose(place, slope_x)
            place = period_ids(stride) - floor_y
            weight_y, deriv_y = choose(place, theta_y), choose(place, slope_y)
            grads = [jnp.zeros((SUBLANES, LANES), jnp.float32) for _ in range(3)]
            for at in range(0, sizes["slab"] + 3, 2):
                sums = [[None] * 3 for _ in range(3)]
                for step in range(2 * stride // SUBLANES):
                    row = at * stride + step * SUBLANES
                    if row >= rows:
                        continue
                    here = slice(row, row + SUBLANES)
                    span = slice(step * SUBLANES, (step + 1) * SUBLANES)
                    along = along_ref[here, block * LANES : (block + 1) * LANES]
                    slope = along_ref[here, lanes + block * LANES : lanes + (block + 1) * LANES]
                    kind = 0 if step < middle else 1 if step == middle else 2
                    terms = (along * weight_y[span], along * deriv_y[span], slope * weight_y[span])
                    for axis in range(3):
                        held = sums[axis][kind]
                        sums[axis][kind] = terms[axis] if held is None else held + terms[axis]
                factors = []
                for table in range(2):
                    first = repeated_row(table_ref, kept + table, at)
                    second = repeated_row(table_ref, kept + table, at + 1)
                    factors.append((first, jnp.where(low_half, first, second), second))
                for axis, table in enumerate((1, 0, 0)):
                    for kind in range(3):
                        grads[axis] = grads[axis] + sums[axis][kind] * factors[table][kind]
            charge = parts[2] * scale
            for axis in range(3):
                row = jnp.sum(grads[axis], axis=0, keepdims=True) * charge
                out_ref[axis, pl.ds(tile, 1), :] = row

    set_a, set_b = (along_a, weight_a), (along_b, weight_b)
    contract_z(0, *set_a)

    def two_chunks(step, carry):
        contract_z(2 * step + 1, *set_b)
        finish(2 * step, 0, along_a)
        contract_z(2 * step + 2, *set_a)
        finish(2 * step + 1, 1, along_b)
        return carry

    lax.fori_loop(0, chunks // 2 - 1, two_chunks, 0)
    contract_z(chunks - 1, *set_b)
    finish(chunks - 2, 0, along_a)
    finish(chunks - 1, 1, along_b)


def pair_kernel(
    listed_ref, near_ref, out_ref, *, factors, scale, domains, pencils, together
):
    tiles = near_ref.shape[2]
    pairs = listed_ref.shape[0] // 2
    dom_at, pen_at = lax.axis_index("dom"), lax.axis_index("pen")
    out_ref[...] = jnp.zeros_like(out_ref)

    def wrapped(seen, count):
        return jnp.where(seen < 0, -1.0, jnp.where(seen >= count, 1.0, 0.0))

    def one_pair(n):
        home = listed_ref[n]
        other = listed_ref[pairs + n]
        around = other // tiles
        tile = other - around * tiles
        step_dom = around // 3
        wrap_x = wrapped(dom_at + step_dom - 1, domains)
        wrap_y = wrapped(pen_at + around - 3 * step_dom - 1, pencils)
        mine = [near_ref[4, part, pl.ds(home, 1), :] for part in range(4)]
        theirs = jnp.concatenate(
            [near_ref[around, part, pl.ds(tile, 1), :] for part in range(4)] * 2, axis=0
        ).T
        delta_x = (mine[0] - wrap_x) - theirs[:, 0:1]
        delta_y = (mine[1] - wrap_y) - theirs[:, 1:2]
        delta_z = mine[2] - theirs[:, 2:3]
        delta_z = delta_z - jnp.floor(delta_z + 0.5)
        scaled = (delta_x * factors[0], delta_y * factors[1], delta_z * factors[2])
        square = scaled[0] * scaled[0] + scaled[1] * scaled[1] + scaled[2] * scaled[2]
        weight = jnp.exp(-0.5 * square) * theirs[:, 3:4]
        charge = mine[3] * scale
        return home, [jnp.sum(part * weight, axis=0, keepdims=True) * charge for part in scaled]

    def some_pairs(step, carry):
        found = [one_pair(step * together + n) for n in range(together)]
        for home, pushes in found:
            for axis in range(3):
                out_ref[axis, pl.ds(home, 1), :] += pushes[axis]
        return carry

    lax.fori_loop(0, pairs // together, some_pairs, 0)


def neighbours(block):
    near = block[None]
    for axis in ("pen", "dom"):
        count = lax.axis_size(axis)
        up = [(i, (i + 1) % count) for i in range(count)]
        down = [(i, (i - 1) % count) for i in range(count)]
        lower = lax.ppermute(near, axis, up)
        upper = lax.ppermute(near, axis, down)
        near = jnp.concatenate([lower, near, upper], axis=0)
    return near


def in_vmem(value):
    return pltpu.with_memory_space_constraint(jnp.asarray(value), pltpu.VMEM)


def whole_spec():
    return pl.BlockSpec(memory_space=pltpu.VMEM)


def smem_spec():
    return pl.BlockSpec(memory_space=pltpu.SMEM)


def fast_on_device(atoms, pair_home, pair_other, *, sizes):
    groups, domains, pencils = sizes["groups"], sizes["domains"], sizes["pencils"]
    rows, share, block = sizes["rows"], sizes["share"], sizes["block"]
    slab, stride = sizes["slab"], sizes["stride"]
    devices = groups * domains * pencils
    atom_count = atoms.shape[3]
    tiles = atom_count // LANES
    own = atoms.reshape(4, tiles, LANES)
    freq, basis = real_basis()
    order = (np.arange(domains)[None, :] * slab + np.arange(slab)[:, None]).reshape(-1)
    mixed = np.ascontiguousarray(basis[:, order])
    line = line_factor(freq)
    plane = in_vmem((line[:, None] * line[None, :] / np.pi).astype(np.float32))
    plane_sq = in_vmem((freq[:, None] ** 2 + freq[None, :] ** 2).astype(np.float32))
    basis_arr = jnp.asarray(basis)
    kept_basis = in_vmem(basis)
    line_rows = np.zeros((-(-(NG // 2 + 1) // SUBLANES) * SUBLANES, LANES), np.float32)
    line_rows[: NG // 2 + 1] = line[: NG // 2 + 1, None]
    message = pltpu.VMEM((devices, share, rows), jnp.float32)

    nearby = in_vmem(neighbours(own))

    chunk = 512
    charge = pl.pallas_call(
        lambda *refs: spread_kernel(*refs, sizes=sizes),
        in_specs=[whole_spec(), whole_spec()],
        out_specs=whole_spec(),
        out_shape=message,
        scratch_shapes=[
            pltpu.VMEM((rows, 3 * NG), jnp.float32),
            pltpu.VMEM((2 * chunk // LANES, stride + 4, LANES), jnp.float32),
        ]
        + [
            pltpu.VMEM((rows, chunk), jnp.bfloat16),
            pltpu.VMEM((rows, chunk), jnp.bfloat16),
            pltpu.VMEM((2 * NG, chunk), jnp.bfloat16),
        ]
        * 2,
        grid=(),
        name="spread",
    )(basis_arr, own)

    def exchange(value):
        value = lax.all_to_all(value, MESH_AXES, split_axis=0, concat_axis=0, tiled=True)
        return in_vmem(value)

    received = exchange(charge)
    returned = pl.pallas_call(
        lambda *refs: spectral_kernel(*refs, sizes=sizes),
        in_specs=[whole_spec()]
        + [whole_spec()] * 5
        + [whole_spec()],
        out_specs=whole_spec(),
        out_shape=message,
        scratch_shapes=[
            pltpu.VMEM((pencils * block, rows), jnp.float32),
            pltpu.VMEM((slab * block, NG), jnp.float32),
        ],
        grid=(),
        name="spectral",
    )(
        in_vmem(line_rows),
        kept_basis,
        in_vmem(mixed),
        in_vmem(mixed.T),
        plane,
        plane_sq,
        received,
    )
    coefs = exchange(returned)

    out_shape = jax.ShapeDtypeStruct((3, tiles, LANES), jnp.float32)
    pairs = pair_home.size
    short_out = pl.pallas_call(
        lambda *refs: pair_kernel(
            *refs,
            factors=(2.0 * domains, 2.0 * pencils, 2.0 * domains),
            scale=2.0 / math.sqrt(atom_count / domains),
            domains=domains,
            pencils=pencils,
            together=math.gcd(4, pairs),
        ),
        in_specs=[smem_spec(), whole_spec()],
        out_specs=whole_spec(),
        out_shape=out_shape,
        grid=(),
        name="pairs",
    )(jnp.concatenate([pair_home.reshape(-1), pair_other.reshape(-1)]), nearby)

    chunk = 256
    long_scale = -0.4 * NG / math.sqrt(NG * atom_count * devices)
    long_out = pl.pallas_call(
        lambda *refs: interpolate_kernel(*refs, sizes=sizes, scale=long_scale),
        in_specs=[whole_spec(), whole_spec(), whole_spec()],
        out_specs=whole_spec(),
        out_shape=out_shape,
        scratch_shapes=[
            pltpu.VMEM((rows, 3 * NG), jnp.bfloat16),
            pltpu.VMEM((4 * chunk // LANES, stride + 4, LANES), jnp.float32),
        ]
        + [
            pltpu.VMEM((rows, 2 * chunk), jnp.float32),
            pltpu.VMEM((3 * NG, 2 * chunk), jnp.bfloat16),
        ]
        * 2,
        grid=(),
        name="interpolate",
    )(kept_basis, coefs, in_vmem(own))
    return (short_out.reshape(3, 1, 1, atom_count), long_out.reshape(3, 1, 1, atom_count))


def solution(mesh):
    placed = (P(None, "grp", "dom", "pen"), P("grp", "dom", "pen"), P("grp", "dom", "pen"))

    def body(atoms, pair_home, pair_other):
        sizes = fast_sizes(
            mesh.shape["grp"], mesh.shape["dom"], mesh.shape["pen"], atoms.shape[3]
        )
        if sizes is None:
            return on_device(atoms, pair_home, pair_other)
        return fast_on_device(atoms, pair_home, pair_other, sizes=sizes)

    return jax.shard_map(
        body,
        mesh=mesh,
        in_specs=placed,
        out_specs=(P(None, "grp", "dom", "pen"), P(None, "grp", "dom", "pen")),
        check_vma=False,
    )
```
